32 devices in a mesh: dp: 1 (over z), tp: 4 (over y), wg: 8 (over x, core).
Axes of the slice: x: 4, y: 4, z: 1, core: 2. Of those that a mesh axis runs over, the one named last changes fastest.
The devices are a block of a 4x4x8 slice.
Arguments:
- tokens: bfloat16 [8192, 1024], P(('dp', 'wg'))
- gain_attn: float32 [1024], P('wg')
- gain_mlp: float32 [1024], P('wg')
- w_qkv: bfloat16 [1024, 3, 16, 64], P('wg', None, 'tp')
- w_rel: bfloat16 [1024, 16, 64], P('wg', 'tp')
- w_out: bfloat16 [16, 64, 1024], P('tp', None, 'wg')
- w_up: bfloat16 [1024, 4096], P('wg', 'tp')
- w_down: bfloat16 [4096, 1024], P('tp', 'wg')
- bias_u: float32 [16, 64], P('tp')
- bias_v: float32 [16, 64], P('tp')
- rel_table: bfloat16 [8, 1024], replicated
- k_cache: bfloat16 [8192, 16, 8, 64], P(('dp', 'wg'), 'tp')
- v_cache: bfloat16 [8192, 16, 8, 64], P(('dp', 'wg'), 'tp')
- positions: int32 [8192], P(('dp', 'wg'))
Outputs:
- output 1: bfloat16 [8192, 1024], P(('dp', 'wg'))
- output 2: bfloat16 [8192, 16, 64], P(('dp', 'wg'), 'tp')
- output 3: bfloat16 [8192, 16, 64], P(('dp', 'wg'), 'tp')
All inputs are finite; a program needn't handle non-finite values.
Results may differ from the reference program's by a relative error of at most 0.0131761.
Values are sent between devices in bfloat16 or wider.
A program may use at most 768 MiB of HBM per device.

```python
import math
import jax
import jax.numpy as jnp
from jax import lax

D_MODEL = 1024
N_HEADS = 16
HEAD_DIM = 64
FF_DIM = 4096
CACHE_LEN = 8
SEQ_COUNT = 8192
SEQ_BLOCK = 8
NORM_EPS = 1e-6
SCORE_SCALE = 1.0 / math.sqrt(HEAD_DIM)
BLOCK_COUNT = SEQ_COUNT // SEQ_BLOCK


def setup_inputs(seed: int = 0, part: int = 0) -> dict:
    base_key = jax.random.key(seed)
    part_key = jax.random.fold_in(base_key, part)
    weight_keys = jax.random.split(base_key, 12)
    part_keys = jax.random.split(part_key, 4)
    head_width = N_HEADS * HEAD_DIM
    gain_attn = jax.random.uniform(weight_keys[0], (D_MODEL,), jnp.float32, 0.5, 1.5)
    gain_mlp = jax.random.uniform(weight_keys[1], (D_MODEL,), jnp.float32, 0.5, 1.5)
    w_qkv = (jax.random.normal(weight_keys[2], (D_MODEL, 3, N_HEADS, HEAD_DIM), jnp.float32) * D_MODEL ** -0.5).astype(jnp.bfloat16)
    w_rel = (jax.random.normal(weight_keys[3], (D_MODEL, N_HEADS, HEAD_DIM), jnp.float32) * (2.0 / D_MODEL) ** 0.5).astype(jnp.bfloat16)
    w_out = (jax.random.normal(weight_keys[4], (N_HEADS, HEAD_DIM, D_MODEL), jnp.float32) * 2.0 * head_width ** -0.5).astype(jnp.bfloat16)
    w_up = (jax.random.normal(weight_keys[5], (D_MODEL, FF_DIM), jnp.float32) * D_MODEL ** -0.5).astype(jnp.bfloat16)
    w_down = (jax.random.normal(weight_keys[6], (FF_DIM, D_MODEL), jnp.float32) * FF_DIM ** -0.5).astype(jnp.bfloat16)
    bias_u = jax.random.normal(weight_keys[7], (N_HEADS, HEAD_DIM), jnp.float32)
    bias_v = jax.random.normal(weight_keys[8], (N_HEADS, HEAD_DIM), jnp.float32)
    rel_freqs = jnp.exp(jax.random.uniform(weight_keys[9], (D_MODEL,), jnp.float32, math.log(0.01), math.log(3.0)))
    phases = jax.random.uniform(weight_keys[10], (D_MODEL,), jnp.float32, 0.0, 2.0 * math.pi)
    offsets = jnp.arange(CACHE_LEN, dtype=jnp.float32)
    rel_table = jnp.sin(offsets[:, None] * rel_freqs[None, :] + phases[None, :]).astype(jnp.bfloat16)
    tokens = jax.random.normal(part_keys[0], (SEQ_COUNT, D_MODEL), jnp.float32).astype(jnp.bfloat16)
    k_cache = jax.random.normal(part_keys[1], (SEQ_COUNT, N_HEADS, CACHE_LEN, HEAD_DIM), jnp.float32).astype(jnp.bfloat16)
    v_cache = jax.random.normal(part_keys[2], (SEQ_COUNT, N_HEADS, CACHE_LEN, HEAD_DIM), jnp.float32).astype(jnp.bfloat16)
    positions = jax.random.randint(part_keys[3], (SEQ_COUNT,), 0, CACHE_LEN, jnp.int32)
    positions = positions.at[0].set(CACHE_LEN - 1)
    return {"tokens": tokens, "gain_attn": gain_attn, "gain_mlp": gain_mlp, "w_qkv": w_qkv, "w_rel": w_rel, "w_out": w_out, "w_up": w_up, "w_down": w_down, "bias_u": bias_u, "bias_v": bias_v, "rel_table": rel_table, "k_cache": k_cache, "v_cache": v_cache, "positions": positions}


def rms_norm(row_vals, gain_vec):
    vals_f32 = row_vals.astype(jnp.float32)
    mean_sq = jnp.mean(vals_f32 * vals_f32, axis=-1, keepdims=True)
    return (vals_f32 * lax.rsqrt(mean_sq + NORM_EPS) * gain_vec).astype(jnp.bfloat16)


def attend_block(block_args, rel_f32):
    q_u, q_v, k_new, v_new, k_blk, v_blk, pos_blk = block_args
    key_steps = jnp.arange(CACHE_LEN)
    is_self = key_steps[None, :] == pos_blk[:, None]
    is_valid = key_steps[None, :] <= pos_blk[:, None]
    k_full = jnp.where(is_self[:, None, :, None], k_new[:, :, None, :], k_blk).astype(jnp.float32)
    v_full = jnp.where(is_self[:, None, :, None], v_new[:, :, None, :], v_blk).astype(jnp.float32)
    content = jnp.einsum("bhe,bhje->bhj", q_u.astype(jnp.float32), k_full)
    rel_all = jnp.einsum("bhe,rhe->bhr", q_v.astype(jnp.float32), rel_f32)
    rel_index = jnp.clip(pos_blk[:, None] - key_steps[None, :], 0, CACHE_LEN - 1)
    rel_scores = jnp.take_along_axis(rel_all, jnp.broadcast_to(rel_index[:, None, :], rel_all.shape), axis=2)
    scores = jnp.where(is_valid[:, None, :], (content + rel_scores) * SCORE_SCALE, -1e30)
    attn_probs = jax.nn.softmax(scores, axis=-1).astype(jnp.bfloat16)
    attn_out = jnp.einsum("bhj,bhje->bhe", attn_probs.astype(jnp.float32), v_full)
    return attn_out.astype(jnp.bfloat16)


def reference(tokens, gain_attn, gain_mlp, w_qkv, w_rel, w_out, w_up, w_down, bias_u, bias_v, rel_table, k_cache, v_cache, positions):
    head_width = N_HEADS * HEAD_DIM
    normed = rms_norm(tokens, gain_attn)
    qkv_heads = jnp.dot(normed, w_qkv.reshape(D_MODEL, 3 * head_width), preferred_element_type=jnp.float32).astype(jnp.bfloat16).reshape(SEQ_COUNT, 3, N_HEADS, HEAD_DIM)
    q_heads = qkv_heads[:, 0]
    k_new = qkv_heads[:, 1]
    v_new = qkv_heads[:, 2]
    rel_proj = jnp.dot(rel_table, w_rel.reshape(D_MODEL, head_width), preferred_element_type=jnp.float32).astype(jnp.bfloat16).reshape(CACHE_LEN, N_HEADS, HEAD_DIM)
    rel_f32 = rel_proj.astype(jnp.float32)
    q_u = (q_heads.astype(jnp.float32) + bias_u).astype(jnp.bfloat16)
    q_v = (q_heads.astype(jnp.float32) + bias_v).astype(jnp.bfloat16)

    def to_blocks(array_in):
        return array_in.reshape((BLOCK_COUNT, SEQ_BLOCK) + array_in.shape[1:])

    def run_block(block_args):
        return attend_block(block_args, rel_f32)

    blocked = tuple(to_blocks(array_in) for array_in in (q_u, q_v, k_new, v_new, k_cache, v_cache, positions))
    attn_out = lax.map(run_block, blocked)
    attn_flat = attn_out.reshape(SEQ_COUNT, head_width)
    attn_proj = jnp.dot(attn_flat, w_out.reshape(head_width, D_MODEL), preferred_element_type=jnp.float32)
    resid = tokens.astype(jnp.float32) + attn_proj
    normed_mlp = rms_norm(resid, gain_mlp)
    hidden = jax.nn.gelu(jnp.dot(normed_mlp, w_up, preferred_element_type=jnp.float32), approximate=True).astype(jnp.bfloat16)
    layer_out = (resid + jnp.dot(hidden, w_down, preferred_element_type=jnp.float32)).astype(jnp.bfloat16)
    return (layer_out, k_new, v_new)
```

```python
import functools

import jax
import jax.numpy as jnp
from jax import lax
from jax.experimental import pallas as pl
from jax.experimental.pallas import tpu as pltpu
from jax.sharding import PartitionSpec as P

NORM_EPS = 1e-6
CORES = 2
CHUNK = 256
MAX_SENDS = 136
MAX_LOCALS = 24
F32, BF16 = jnp.float32, jnp.bfloat16


def dot_nn(a, b):
    return lax.dot_general(a, b, (((1,), (0,)), ((), ())), preferred_element_type=F32)


def dot_nt(a, b):
    return lax.dot_general(a, b, (((1,), (1,)), ((), ())), preferred_element_type=F32)


def aligned(start, size):
    return pl.ds(pl.multiple_of(start, size), size)


def layer_kernel(n_wg, n_tp, dims, tok_hbm, ga_hbm, gm_hbm, wq_hbm, wr_hbm, wo_hbm, wu_hbm, wd_hbm, bu_ref, bv_ref, rt_ref, kc_hbm, vc_hbm, pos_ref,
                 y_hbm, kn_hbm, vn_hbm,
                 tok, kc, vc, gbuf, wqr, wout, wup, wdn, normed, qkv, rel, relp, rels, obuf, otr, hid, z, ybuf, sends, recvs, locs):
    heads, slots, e_dim = dims
    n_tok, d = tok.shape
    he = heads * e_dim
    f_loc = wu_hbm.shape[1]
    piece = d // n_wg
    n_x = n_wg // CORES
    n_chunk = n_tok // CHUNK
    me = lax.axis_index("wg")
    x, c = me // CORES, lax.rem(me, CORES)
    y = lax.axis_index("tp")

    def at_x(off):
        return lax.rem(x + off + n_x, n_x)

    def wg_of(off, core):
        return at_x(off) * CORES + core

    def at_y(off):
        return lax.rem(y + off + n_tp, n_tp)

    other = 1 - c
    dev = {"x+": {"wg": wg_of(1, c)}, "x-": {"wg": wg_of(-1, c)}, "sib": {"wg": x * CORES + other}, "y+": {"tp": at_y(1)}, "y-": {"tp": at_y(-1)}}

    ids, pending = {}, []

    def sem(name):
        return ids.setdefault(name, len(ids))

    def remote(name, view, to):
        i = sem(name)
        return pltpu.make_async_remote_copy(src_ref=view, dst_ref=view, send_sem=sends.at[i], recv_sem=recvs.at[i], device_id=dev[to], device_id_type=pl.DeviceIdType.MESH)

    def send(name, view, to):
        copy = remote(name, view, to)
        copy.start()
        pending.append(copy)

    def recv(name, view, frm="sib"):
        remote(name, view, frm).wait_recv()

    n_local = [0]

    def local(src, dst):
        copy = pltpu.make_async_copy(src, dst, locs.at[n_local[0]])
        n_local[0] += 1
        copy.start()
        return copy

    def x_own(t, view):
        v = view(at_x(0), c, None)
        send(t + "r", v, "x+")
        send(t + "l", v, "x-")
        send(t + "s0", v, "sib")

    def x_relay(t, view, then=None):
        recv(t + "r", view(at_x(-1), c, None))
        send(t + "r2", view(at_x(-1), c, 0), "x+")
        recv(t + "l", view(at_x(1), c, None))
        send(t + "l2", view(at_x(1), c, 1), "x-")
        send(t + "s1", view(at_x(-1), c, None), "sib")
        send(t + "s2", view(at_x(1), c, None), "sib")

    def x_fin(t, view):
        recv(t + "r2", view(at_x(2), c, 0))
        send(t + "s3", view(at_x(2), c, 0), "sib")
        recv(t + "l2", view(at_x(2), c, 1))
        send(t + "s4", view(at_x(2), c, 1), "sib")

    def x_sib(t, view):
        recv(t + "s0", view(at_x(0), other, None))
        recv(t + "s1", view(at_x(-1), other, None))
        recv(t + "s2", view(at_x(1), other, None))
        recv(t + "s3", view(at_x(2), other, 0))
        recv(t + "s4", view(at_x(2), other, 1))

    def y_own(t, view):
        v = view(at_y(0), None, c)
        send(t + "r", v, "y+")
        send(t + "l", v, "y-")

    def y_relay(t, view, share=False):
        recv(t + "r", view(at_y(-1), None, c))
        send(t + "r2", view(at_y(-1), 0, c), "y+")
        recv(t + "l", view(at_y(1), None, c))
        send(t + "l2", view(at_y(1), 1, c), "y-")
        if share:
            send(t + "s1", view(at_y(-1), None, c), "sib")
            send(t + "s2", view(at_y(1), None, c), "sib")

    def y_fin(t, view, share=False):
        recv(t + "r2", view(at_y(2), 0, c))
        if share:
            send(t + "s3", view(at_y(2), 0, c), "sib")
        recv(t + "l2", view(at_y(2), 1, c))
        if share:
            send(t + "s4", view(at_y(2), 1, c), "sib")

    def y_sib_near(t, view):
        recv(t + "s1", view(at_y(-1), None, other))
        recv(t + "s2", view(at_y(1), None, other))

    def y_sib_far(t, view):
        recv(t + "s3", view(at_y(2), 0, other))
        recv(t + "s4", view(at_y(2), 1, other))

    def rows_of(start, size, half):
        if half is None:
            return aligned(start, size)
        return aligned(start + half * (size // 2), size // 2)

    def gain_view(xi, core, half):
        w = xi * CORES + core
        return gbuf.at[w] if half is None else gbuf.at[w, pl.ds(half, 1)]

    def col_view(ref, row0, n_rows):
        def view(xi, core, half):
            return ref.at[rows_of(row0, n_rows, half), aligned((xi * CORES + core) * piece, piece)]
        return view

    wqr_view = col_view(wqr, 0, wqr.shape[0])
    out_view = col_view(wout, 0, wout.shape[0])

    def outy_view(yi, half, core):
        return wout.at[rows_of(yi * he, he, half), aligned((x * CORES + core) * piece, piece)]

    def dny_view(yi, half, core):
        return wdn.at[rows_of(yi * f_loc, f_loc, half), aligned((x * CORES + core) * piece, piece)]

    def dn_view(off):
        return col_view(wdn, at_y(off) * f_loc, f_loc)

    def up_view(xi, core, half):
        return wup.at[rows_of(at_y(0) * d + (xi * CORES + core) * piece, piece, half)]

    def upy_view(off):
        def view(yi, half, core):
            return wup.at[rows_of(yi * d + (at_x(off) * CORES + core) * piece, piece, half)]
        return view

    def o_view(ch):
        def view(yi, half, core):
            return obuf.at[rows_of(ch * CHUNK, CHUNK, half), aligned(yi * he, he)]
        return view

    own_cols = aligned(me * piece, piece)
    n_qkv = wq_hbm.shape[0]
    l_g = [local(ga_hbm, gbuf.at[me, pl.ds(0, 1)]), local(gm_hbm, gbuf.at[me, pl.ds(1, 1)])]
    l_w = [local(wq_hbm, wqr.at[pl.ds(0, n_qkv), own_cols]), local(wr_hbm, wqr.at[pl.ds(n_qkv, he), own_cols])]
    l_o = local(wo_hbm, wout.at[aligned(y * he, he), own_cols])
    l_t = local(tok_hbm, tok)
    l_d = local(wd_hbm, wdn.at[aligned(y * f_loc, f_loc), own_cols])
    l_u = local(wu_hbm, wup.at[aligned(y * d + me * piece, piece)])
    l_k = local(kc_hbm, kc)
    l_v = local(vc_hbm, vc)

    barrier = pltpu.get_barrier_semaphore()
    for to in dev.values():
        pl.semaphore_signal(barrier, inc=1, device_id=to, device_id_type=pl.DeviceIdType.MESH)
    pl.semaphore_wait(barrier, len(dev))

    for copy in l_g:
        copy.wait()
    x_own("g", gain_view)
    for copy in l_w:
        copy.wait()
    x_own("q", wqr_view)
    l_o.wait()
    y_own("oy", outy_view)
    l_d.wait()
    y_own("dy", dny_view)
    x_relay("g", gain_view)
    y_relay("oy", outy_view)
    x_fin("g", gain_view)
    x_sib("g", gain_view)
    l_t.wait()

    def gain_row(i):
        return jnp.concatenate([gbuf[w, i:i + 1, :] for w in range(n_wg)], axis=1)

    def norm(vals, gain):
        mean_sq = jnp.mean(vals * vals, axis=-1, keepdims=True)
        return (vals * lax.rsqrt(mean_sq + NORM_EPS) * gain).astype(BF16)

    norm_rows = 64

    @pl.loop(0, n_tok // norm_rows)
    def _(i):
        r = aligned(i * norm_rows, norm_rows)
        normed[r, :] = norm(tok[r, :].astype(F32), gain_row(0))

    y_fin("oy", outy_view)
    x_relay("q", wqr_view)
    x_own("o", out_view)
    y_relay("dy", dny_view)
    l_u.wait()
    y_own("u0", upy_view(0))
    x_fin("q", wqr_view)
    x_sib("q", wqr_view)

    n_rel = slots * heads * slots
    row = lax.broadcasted_iota(jnp.int32, (n_rel, slots), 0)
    col = lax.broadcasted_iota(jnp.int32, (n_rel, slots), 1)
    offset = jnp.maximum(row // (heads * slots) - lax.rem(row, slots), 0)
    pick = jnp.where(col == offset, 1.0, 0.0).astype(BF16)
    table = dot_nn(pick, rt_ref[...]).astype(BF16)
    rel_q = dot_nt(table, wqr[n_qkv:n_qkv + he, :]).astype(BF16).astype(F32)
    row = lax.broadcasted_iota(jnp.int32, (n_rel, he), 0)
    col = lax.broadcasted_iota(jnp.int32, (n_rel, he), 1)
    relp[...] = jnp.where(lax.rem(row // slots, heads) == col // e_dim, rel_q, 0.0).astype(BF16)

    eye = lax.broadcasted_iota(jnp.int32, (e_dim, e_dim), 0) == lax.broadcasted_iota(jnp.int32, (e_dim, e_dim), 1)

    def bias_col(ref, h):
        return jnp.sum(jnp.where(eye, ref[h:h + 1, :], 0.0), axis=1, keepdims=True)

    l_k.wait()
    l_v.wait()
    scale = e_dim ** -0.5

    def attend(ch):
        cols = pl.ds(ch * CHUNK, CHUNK)
        pos = pos_ref[:, ch * CHUNK:(ch + 1) * CHUNK]
        chunk = normed[ch * CHUNK:(ch + 1) * CHUNK, :]
        qkv[:, cols] = dot_nt(wqr[0:n_qkv, :], chunk).astype(BF16)
        for h in range(heads):
            q = qkv[h * e_dim:(h + 1) * e_dim, cols].astype(F32)
            rel[h * e_dim:(h + 1) * e_dim, :] = (q + bias_col(bv_ref, h)).astype(BF16)
            otr[h * e_dim:(h + 1) * e_dim, :] = (q + bias_col(bu_ref, h)).astype(BF16).astype(F32)
        rel_all = dot_nn(relp[...], rel[...])
        per_p = heads * slots
        sel = jnp.zeros((per_p, CHUNK), F32)
        for p in range(slots):
            sel = jnp.where(pos == p, rel_all[p * per_p:(p + 1) * per_p, :], sel)
        rels[...] = sel

        @pl.loop(0, heads)
        def _(h):
            r = aligned(h * e_dim, e_dim)
            qu = otr[r, :]
            k_new = qkv[aligned(he + h * e_dim, e_dim), cols].astype(F32)
            v_new = qkv[aligned(2 * he + h * e_dim, e_dim), cols].astype(F32)
            rel_h = rels[aligned(h * slots, slots), :]
            self_s = jnp.sum(qu * k_new, axis=0, keepdims=True)
            scores = []
            for j in range(slots):
                s = jnp.sum(qu * kc[h, j, :, cols].astype(F32), axis=0, keepdims=True)
                s = (jnp.where(pos == j, self_s, s) + rel_h[j:j + 1, :]) * scale
                scores.append(jnp.where(pos >= j, s, -1e30))
            top = functools.reduce(jnp.maximum, scores)
            exps = [jnp.exp(s - top) for s in scores]
            total = functools.reduce(jnp.add, exps)
            self_a = jnp.zeros_like(total)
            out = jnp.zeros((e_dim, CHUNK), F32)
            for j in range(slots):
                a = (exps[j] / total).astype(BF16).astype(F32)
                self_a = jnp.where(pos == j, a, self_a)
                out = out + jnp.where(pos > j, a, 0.0) * vc[h, j, :, cols].astype(F32)
            otr[r, :] = out + self_a * v_new

        obuf[ch * CHUNK:(ch + 1) * CHUNK, aligned(y * he, he)] = otr[...].T.astype(BF16)

    def project(ch):
        r = pl.ds(ch * CHUNK, CHUNK)
        hid[r, :] = tok[r, :].astype(F32) + dot_nn(obuf[r, :], wout[...])
        gain = gain_row(1)

        @pl.loop(0, CHUNK // norm_rows)
        def _(i):
            q = aligned(ch * CHUNK + i * norm_rows, norm_rows)
            normed[q, :] = norm(hid[q, :], gain)

    attend(0)
    y_own("a0", o_view(0))
    x_relay("o", out_view)
    x_own("u", up_view)
    attend(1)
    y_own("a1", o_view(1))
    y_relay("a0", o_view(0))
    y_fin("dy", dny_view)
    attend(2)
    y_own("a2", o_view(2))
    y_relay("a1", o_view(1))
    x_fin("o", out_view)
    attend(3)
    y_own("a3", o_view(3))
    y_relay("a2", o_view(2))
    l_kn = local(qkv.at[pl.ds(he, he)], kn_hbm)
    l_vn = local(qkv.at[pl.ds(2 * he, he)], vn_hbm)
    x_relay("u", up_view)
    x_own("d0", dn_view(0))
    x_own("d1", dn_view(-1))
    x_sib("o", out_view)
    y_fin("a0", o_view(0))
    project(0)
    y_relay("a3", o_view(3))
    y_own("u1", upy_view(-1))
    y_own("u2", upy_view(1))
    y_fin("a1", o_view(1))
    project(1)
    x_fin("u", up_view)
    y_own("u3", upy_view(2))
    y_relay("u0", upy_view(0), True)
    y_fin("a2", o_view(2))
    project(2)
    x_sib("u", up_view)
    y_fin("a3", o_view(3))
    project(3)

    def up(off):
        base = at_y(off) * d

        @pl.loop(0, n_chunk)
        def _(i):
            r = aligned(i * CHUNK, CHUNK)
            acc = dot_nn(normed[r, :], wup[aligned(base, d), :])
            z[r, :] = jax.nn.gelu(acc, approximate=True).astype(BF16)

    def down(off):
        base = at_y(off) * f_loc

        @pl.loop(0, n_chunk)
        def _(i):
            r = aligned(i * CHUNK, CHUNK)
            hid[r, :] += dot_nn(z[r, :], wdn[aligned(base, f_loc), :])

    up(0)
    x_relay("d0", dn_view(0))
    x_own("d2", dn_view(1))
    y_relay("u1", upy_view(-1), True)
    y_fin("u0", upy_view(0), True)
    x_fin("d0", dn_view(0))
    x_relay("d1", dn_view(-1))
    x_own("d3", dn_view(2))
    x_sib("d0", dn_view(0))
    down(0)
    y_relay("u2", upy_view(1), True)
    x_fin("d1", dn_view(-1))
    y_fin("u1", upy_view(-1), True)
    y_relay("u3", upy_view(2), True)
    x_relay("d2", dn_view(1))
    for k, off in enumerate((0, -1, 1, 2)):
        y_sib_near("u%d" % k, upy_view(off))
    up(-1)
    x_sib("d1", dn_view(-1))
    x_fin("d2", dn_view(1))
    y_fin("u2", upy_view(1), True)
    down(-1)
    x_relay("d3", dn_view(2))
    y_fin("u3", upy_view(2), True)
    up(1)
    x_fin("d3", dn_view(2))
    x_sib("d2", dn_view(1))
    down(1)
    for k, off in enumerate((0, -1, 1, 2)):
        y_sib_far("u%d" % k, upy_view(off))
    up(2)
    x_sib("d3", dn_view(2))
    base = at_y(2) * f_loc
    outs = []
    for i in range(n_chunk):
        r = pl.ds(i * CHUNK, CHUNK)
        ybuf[r, :] = (hid[r, :] + dot_nn(z[r, :], wdn[aligned(base, f_loc), :])).astype(BF16)
        outs.append(local(ybuf.at[r], y_hbm.at[r]))
    for copy in pending:
        copy.wait_send()
    for copy in [l_kn, l_vn] + outs:
        copy.wait()


def solution(mesh):
    tok_axes = ("dp", "wg")
    in_specs = (P(tok_axes, None), P("wg"), P("wg"), P("wg", None, "tp", None), P("wg", "tp", None), P("tp", None, "wg"), P("wg", "tp"), P("tp", "wg"), P("tp", None), P("tp", None), P(None, None), P(tok_axes, "tp", None, None), P(tok_axes, "tp", None, None), P(tok_axes))
    out_specs = (P(tok_axes, None), P(tok_axes, "tp", None), P(tok_axes, "tp", None))
    n_wg, n_tp = mesh.shape["wg"], mesh.shape["tp"]

    def device_step(tokens, gain_attn, gain_mlp, w_qkv, w_rel, w_out, w_up, w_down, bias_u, bias_v, rel_table, k_cache, v_cache, positions):
        n_tok, d = tokens.shape
        _, heads, slots, e_dim = k_cache.shape
        he = heads * e_dim
        piece, f_loc = w_up.shape
        w_q = jnp.transpose(w_qkv, (1, 2, 3, 0)).reshape(3 * he, piece)
        w_r = jnp.transpose(w_rel, (1, 2, 0)).reshape(he, piece)
        w_o = w_out.reshape(he, piece)
        k_t = jnp.transpose(k_cache, (1, 2, 3, 0))
        v_t = jnp.transpose(v_cache, (1, 2, 3, 0))
        hbm = pl.BlockSpec(memory_space=pl.ANY)
        vmem = pl.BlockSpec(memory_space=pltpu.VMEM)
        y, k_new, v_new = pl.pallas_call(
            functools.partial(layer_kernel, n_wg, n_tp, (heads, slots, e_dim)),
            out_shape=(jax.ShapeDtypeStruct((n_tok, d), BF16), jax.ShapeDtypeStruct((he, n_tok), BF16), jax.ShapeDtypeStruct((he, n_tok), BF16)),
            in_specs=[hbm] * 8 + [vmem] * 3 + [hbm] * 2 + [vmem],
            out_specs=(hbm, hbm, hbm),
            scratch_shapes=[
                pltpu.VMEM((n_tok, d), BF16),
                pltpu.VMEM(k_t.shape, BF16),
                pltpu.VMEM(v_t.shape, BF16),
                pltpu.VMEM((n_wg, 2, piece), F32),
                pltpu.VMEM((4 * he, d), BF16),
                pltpu.VMEM((n_tp * he, d), BF16),
                pltpu.VMEM((n_tp * d, f_loc), BF16),
                pltpu.VMEM((n_tp * f_loc, d), BF16),
                pltpu.VMEM((n_tok, d), BF16),
                pltpu.VMEM((3 * he, n_tok), BF16),
                pltpu.VMEM((he, CHUNK), BF16),
                pltpu.VMEM((slots * heads * slots, he), BF16),
                pltpu.VMEM((heads * slots, CHUNK), F32),
                pltpu.VMEM((n_tok, n_tp * he), BF16),
                pltpu.VMEM((he, CHUNK), F32),
                pltpu.VMEM((n_tok, d), F32),
                pltpu.VMEM((n_tok, f_loc), BF16),
                pltpu.VMEM((n_tok, d), BF16),
                pltpu.SemaphoreType.DMA((MAX_SENDS,)),
                pltpu.SemaphoreType.DMA((MAX_SENDS,)),
                pltpu.SemaphoreType.DMA((MAX_LOCALS,)),
            ],
            compiler_params=pltpu.CompilerParams(collective_id=0, has_side_effects=True, vmem_limit_bytes=67043328),
            name="decoder_layer",
        )(tokens, gain_attn.reshape(1, piece), gain_mlp.reshape(1, piece), w_q, w_r, w_o, w_up, w_down, bias_u, bias_v, rel_table, k_t, v_t, positions.reshape(1, n_tok))
        k_new = jnp.transpose(k_new.reshape(heads, e_dim, n_tok), (2, 0, 1))
        v_new = jnp.transpose(v_new.reshape(heads, e_dim, n_tok), (2, 0, 1))
        return y, k_new, v_new

    return jax.shard_map(device_step, mesh=mesh, in_specs=in_specs, out_specs=out_specs, check_vma=False)
```

```python
import functools

import jax
import jax.numpy as jnp
from jax import lax
from jax.experimental import pallas as pl
from jax.experimental.pallas import tpu as pltpu
from jax.sharding import PartitionSpec as P

NORM_EPS = 1e-6
CORES = 2
CHUNK = 256
PAIR = 2 * CHUNK
BLOCKS = 4
PARTS = 4
FAMILY_TENSORS, FAMILY_ARRIVALS = 12, 48
TENSORS, ARRIVALS = 21, 80
MAX_LOCALS = 12
F32, BF16 = jnp.float32, jnp.bfloat16


def dot_nn(a, b):
    return lax.dot_general(a, b, (((1,), (0,)), ((), ())), preferred_element_type=F32)


def dot_nt(a, b):
    return lax.dot_general(a, b, (((1,), (1,)), ((), ())), preferred_element_type=F32)


def aligned(start, size):
    return pl.ds(pl.multiple_of(start, size), size)


def layer_kernel(n_wg, n_tp, dims, tok_hbm, ga_hbm, gm_hbm, wq_hbm, wr_hbm, wo_hbm, wu_hbm, wd_hbm, bu_ref, bv_ref, rt_ref, kc_hbm, vc_hbm, pos_ref,
                 y_hbm, kn_hbm, vn_hbm,
                 tok, kc, vc, gbuf, wqr, wout, wup, wdn, normed, qkv, rel, relp, rels, obuf, otr, hid, z, ybuf, sends, recvs, locs):
    heads, slots, e_dim = dims
    n_tok, d = tok.shape
    he = heads * e_dim
    f_loc = wu_hbm.shape[1]
    piece = d // n_wg
    n_x = n_wg // CORES
    n_chunk = n_tok // CHUNK
    blk = f_loc // BLOCKS
    wide = CORES * piece
    me = lax.axis_index("wg")
    x, c = me // CORES, lax.rem(me, CORES)
    y = lax.axis_index("tp")

    def at_x(off):
        return lax.rem(x + off + 2 * n_x, n_x)

    def wg_of(off, core):
        return at_x(off) * CORES + core

    def at_y(off):
        return lax.rem(y + off + n_tp, n_tp)

    other = 1 - c
    dev = {"x+": {"wg": wg_of(1, c)}, "x-": {"wg": wg_of(-1, c)}, "xx": {"wg": wg_of(2, c)}, "sib": {"wg": x * CORES + other}, "y+": {"tp": at_y(1)}, "y-": {"tp": at_y(-1)}}

    families = {"a": (0, 0, ("r", "l", "f")), "v": (4, 12, ("r", "l", "f", "n", "s")), "d": (8, 32, ("r", "l", "f", "s"))}
    tensors, arrivals = {}, {}

    def sem_ids(t, msg):
        if isinstance(t, tuple):
            tensor, base, msgs = families[t[0]]
            return tensor + t[1], base + t[1] * len(msgs) + msgs.index(msg)
        return FAMILY_TENSORS + tensors.setdefault(t, len(tensors)), FAMILY_ARRIVALS + arrivals.setdefault((t, msg), len(arrivals))

    def remote(t, msg, view, to, dst=None):
        i, k = sem_ids(t, msg)
        return pltpu.make_async_remote_copy(src_ref=view, dst_ref=view if dst is None else dst, send_sem=sends.at[i], recv_sem=recvs.at[k], device_id=dev[to], device_id_type=pl.DeviceIdType.MESH)

    def send(t, msg, view, to, dst=None):
        remote(t, msg, view, to, dst).start()

    def recv(t, msg, view):
        remote(t, msg, view, "sib").wait_recv()

    def sent(t, msg, view):
        remote(t, msg, view, "sib").wait_send()

    n_local = [0]

    def local(src, dst):
        copy = pltpu.make_async_copy(src, dst, locs.at[n_local[0]])
        n_local[0] += 1
        copy.start()
        return copy

    def x_own(t, view):
        v = view(0, c, None)
        send(t, "r", v, "x+", view(0, c, None, 1))
        send(t, "l", v, "x-", view(0, c, None, -1))
        send(t, "s", v, "sib")

    def x_relay(t, view):
        recv(t, "r", view(-1, c, None))
        send(t, "f", view(-1, c, 0), "x+", view(-1, c, 0, 1))
        recv(t, "l", view(1, c, None))
        send(t, "f", view(1, c, 1), "x-", view(1, c, 1, -1))
        send(t, "s", view(-1, c, None), "sib")
        send(t, "s", view(1, c, None), "sib")

    def x_fin(t, view):
        recv(t, "f", view(2, c, None))
        send(t, "s", view(2, c, None), "sib")

    def x_sib(t, view):
        recv(t, "s", view.many(n_x))

    def x_sent(t, view):
        sent(t, "r", view.many(n_x + 3))

    def y_own(t, view):
        v = view(at_y(0), None, c)
        send(t, "r", v, "y+")
        send(t, "l", v, "y-")

    def y_relay(t, view, share=False):
        recv(t, "r", view(at_y(-1), None, c))
        send(t, "f", view(at_y(-1), 0, c), "y+")
        recv(t, "l", view(at_y(1), None, c))
        send(t, "f", view(at_y(1), 1, c), "y-")
        if share:
            send(t, "n", view(at_y(-1), None, c), "sib")
            send(t, "n", view(at_y(1), None, c), "sib")

    def y_fin(t, view, share=False):
        recv(t, "f", view(at_y(2), None, c))
        if share:
            send(t, "s", view(at_y(2), None, c), "sib")

    def y_sib_near(t, view):
        recv(t, "n", view.many(2))

    def y_sib_far(t, view):
        recv(t, "s", view(at_y(2), None, other))

    def y_sent(t, view, share=False):
        sent(t, "r", view.many(6 if share else 3))

    def sized(view, many):
        view.many = many
        return view

    def rows_of(start, size, half):
        if half is None:
            return aligned(start, size)
        return aligned(start + half * (size // 2), size // 2)

    def col_view(ref, row0, n_rows):
        def view(off, core, half, hop=0):
            return ref.at[rows_of(row0, n_rows, half), aligned(wg_of(off, core) * piece, piece)]
        return sized(view, lambda n: ref.at[pl.ds(row0, n_rows), pl.ds(0, n * piece)])

    half_q = wqr.shape[0] // 2
    qa_view = col_view(wqr, 0, half_q)
    qb_view = col_view(wqr, half_q, half_q)
    out_view = col_view(wout, 0, wout.shape[0])

    def outy_view(yi, half, core):
        return wout.at[rows_of(yi * he, he, half), aligned(wg_of(0, core) * piece, piece)]

    sized(outy_view, lambda n: wout.at[pl.ds(0, n * he), pl.ds(0, piece)])

    def dny_view(part):
        rows = f_loc // 2

        def view(yi, half, core):
            return wdn.at[yi, rows_of(part * rows, rows, half), aligned(wg_of(0, core) * piece, piece)]
        return sized(view, lambda n: wdn.at[pl.ds(0, n), pl.ds(part * rows, rows), pl.ds(0, piece)])

    def dn_view(b):
        def view(off, core, half, hop=0):
            return wdn.at[:, rows_of(b * blk, blk, half), aligned(wg_of(off, core) * piece, piece)]
        return sized(view, lambda n: wdn.at[:, aligned(b * blk, blk), pl.ds(0, n * piece)])

    def up_view(off, core, half, hop=0):
        return wup.at[y, (off - hop) % n_x, core, rows_of(0, piece, half)]

    sized(up_view, lambda n: wup.at[y, :, :, :, pl.ds(0, n * f_loc // n_wg)])

    def u0_view(yi, half, core):
        return wup.at[yi, 0, core, rows_of(0, piece, half)]

    sized(u0_view, lambda n: wup.at[pl.ds(0, n // CORES), 0])

    def ub_view(b):
        def view(yi, half, core):
            return wup.at[yi, pl.ds(1, n_x - 1), core, rows_of(0, piece, half), aligned(b * blk, blk)]
        return sized(view, lambda n: wup.at[pl.ds(0, n // CORES), pl.ds(1, n_x - 1), :, :, aligned(b * blk, blk)])

    def o_view(ch):
        def view(yi, half, core):
            return obuf.at[rows_of(ch * CHUNK, CHUNK, half), aligned(yi * he, he)]
        return sized(view, lambda n: obuf.at[aligned(ch * CHUNK, CHUNK), pl.ds(0, n * he)])

    own_cols = aligned(me * piece, piece)
    n_qkv = wq_hbm.shape[0]
    l_g = [local(ga_hbm, gbuf.at[me, pl.ds(0, 1)]), local(gm_hbm, gbuf.at[me, pl.ds(1, 1)])]
    l_w = [local(wq_hbm, wqr.at[pl.ds(0, n_qkv), own_cols]), local(wr_hbm, wqr.at[pl.ds(n_qkv, he), own_cols])]
    l_o = local(wo_hbm, wout.at[aligned(y * he, he), own_cols])
    l_t = local(tok_hbm, tok)
    l_d = local(wd_hbm, wdn.at[y, :, own_cols])
    l_u = local(wu_hbm, wup.at[y, 0, c])
    l_k = local(kc_hbm, kc)
    l_v = local(vc_hbm, vc)

    barrier = pltpu.get_barrier_semaphore()
    for to in dev.values():
        pl.semaphore_signal(barrier, inc=1, device_id=to, device_id_type=pl.DeviceIdType.MESH)
    pl.semaphore_wait(barrier, len(dev))

    for copy in l_g:
        copy.wait()
    for to in ("x+", "x-", "xx"):
        send("g", "f", gbuf.at[me], to)
    send("g", "s", gbuf.at[me], "sib")
    for copy in l_w:
        copy.wait()
    x_own("qa", qa_view)
    x_own("qb", qb_view)
    l_o.wait()
    y_own("oy", outy_view)
    l_d.wait()
    y_own("dya", dny_view(0))
    recv("g", "f", gbuf.at[pl.ds(0, n_x - 1)])
    for k in range(1, n_x):
        send("g", "s", gbuf.at[wg_of(k, c)], "sib")
    y_relay("oy", outy_view)
    y_own("dyb", dny_view(1))
    l_u.wait()
    y_own("u0", u0_view)
    x_relay("qa", qa_view)
    recv("g", "s", gbuf.at[pl.ds(0, n_x)])
    l_t.wait()

    def gain_row(i):
        return jnp.concatenate([gbuf[w, i:i + 1, :] for w in range(n_wg)], axis=1)

    def norm(vals, gain):
        mean_sq = jnp.mean(vals * vals, axis=-1, keepdims=True)
        return (vals * lax.rsqrt(mean_sq + NORM_EPS) * gain).astype(BF16)

    norm_rows = 64

    @pl.loop(0, n_tok // norm_rows)
    def _(i):
        r = aligned(i * norm_rows, norm_rows)
        normed[r, :] = norm(tok[r, :].astype(F32), gain_row(0))

    x_relay("qb", qb_view)
    y_fin("oy", outy_view)
    x_own("o", out_view)
    x_own("u", up_view)
    y_relay("dya", dny_view(0))
    y_relay("dyb", dny_view(1))
    x_fin("qa", qa_view)
    x_fin("qb", qb_view)
    x_sib("qa", qa_view)
    x_sib("qb", qb_view)

    n_rel = slots * heads * slots
    row = lax.broadcasted_iota(jnp.int32, (n_rel, slots), 0)
    col = lax.broadcasted_iota(jnp.int32, (n_rel, slots), 1)
    offset = jnp.maximum(row // (heads * slots) - lax.rem(row, slots), 0)
    pick = jnp.where(col == offset, 1.0, 0.0).astype(BF16)
    table = dot_nn(pick, rt_ref[...]).astype(BF16)
    rel_q = dot_nt(table, wqr[n_qkv:n_qkv + he, :]).astype(BF16).astype(F32)
    row = lax.broadcasted_iota(jnp.int32, (n_rel, he), 0)
    col = lax.broadcasted_iota(jnp.int32, (n_rel, he), 1)
    relp[...] = jnp.where(lax.rem(row // slots, heads) == col // e_dim, rel_q, 0.0).astype(BF16)

    eye = lax.broadcasted_iota(jnp.int32, (e_dim, e_dim), 0) == lax.broadcasted_iota(jnp.int32, (e_dim, e_dim), 1)

    def bias_col(ref, h):
        return jnp.sum(jnp.where(eye, ref[h:h + 1, :], 0.0), axis=1, keepdims=True)

    l_k.wait()
    l_v.wait()
    scale = e_dim ** -0.5

    def attend(ch):
        cols = aligned(ch * CHUNK, CHUNK)
        pos = pos_ref[:, cols]
        chunk = normed[cols, :]
        qkv[:, cols] = dot_nt(wqr[0:n_qkv, :], chunk).astype(BF16)
        for h in range(heads):
            q = qkv[h * e_dim:(h + 1) * e_dim, cols].astype(F32)
            rel[h * e_dim:(h + 1) * e_dim, :] = (q + bias_col(bv_ref, h)).astype(BF16)
            otr[h * e_dim:(h + 1) * e_dim, :] = (q + bias_col(bu_ref, h)).astype(BF16).astype(F32)
        rel_all = dot_nn(relp[...], rel[...])
        per_p = heads * slots
        sel = jnp.zeros((per_p, CHUNK), F32)
        for p in range(slots):
            sel = jnp.where(pos == p, rel_all[p * per_p:(p + 1) * per_p, :], sel)
        rels[...] = sel

        @pl.loop(0, heads)
        def _(h):
            r = aligned(h * e_dim, e_dim)
            qu = otr[r, :]
            k_new = qkv[aligned(he + h * e_dim, e_dim), cols].astype(F32)
            v_new = qkv[aligned(2 * he + h * e_dim, e_dim), cols].astype(F32)
            rel_h = rels[aligned(h * slots, slots), :]
            self_s = jnp.sum(qu * k_new, axis=0, keepdims=True)
            scores = []
            for j in range(slots):
                s = jnp.sum(qu * kc[h, j, :, cols].astype(F32), axis=0, keepdims=True)
                s = (jnp.where(pos == j, self_s, s) + rel_h[j:j + 1, :]) * scale
                scores.append(jnp.where(pos >= j, s, -1e30))
            top = functools.reduce(jnp.maximum, scores)
            exps = [jnp.exp(s - top) for s in scores]
            total = functools.reduce(jnp.add, exps)
            self_a = jnp.zeros_like(total)
            out = jnp.zeros((e_dim, CHUNK), F32)
            for j in range(slots):
                a = (exps[j] / total).astype(BF16).astype(F32)
                self_a = jnp.where(pos == j, a, self_a)
                out = out + jnp.where(pos > j, a, 0.0) * vc[h, j, :, cols].astype(F32)
            otr[r, :] = out + self_a * v_new

        obuf[cols, aligned(y * he, he)] = otr[...].T.astype(BF16)

    def project(pair):
        r = aligned(pair * PAIR, PAIR)
        hid[r, :] = tok[r, :].astype(F32) + dot_nn(obuf[r, :], wout[...])
        gain = gain_row(1)

        @pl.loop(0, PAIR // norm_rows)
        def _(i):
            q = aligned(pair * PAIR + i * norm_rows, norm_rows)
            m = norm(hid[q, :], gain)
            for k in range(n_x):
                normed[q, aligned(lax.rem(k - x + n_x, n_x) * wide, wide)] = m[:, k * wide:(k + 1) * wide]

    def up_rows(r, yi, b):
        cols = aligned(b * blk, blk)
        w = wup[yi, :, :, :, cols].reshape(d, blk)
        z[b, r, aligned(yi * blk, blk)] = jax.nn.gelu(dot_nn(normed[r, :], w), approximate=True).astype(BF16)

    def up_own(pair):
        @pl.loop(0, BLOCKS)
        def _(b):
            up_rows(aligned(pair * PAIR, PAIR), y, b)

    def up_near(b):
        @pl.loop(0, 2)
        def _(i):
            up_rows(slice(None), at_y(2 * i - 1), b)

    def up_far(b):
        up_rows(slice(None), at_y(2), b)

    n_out = 4

    def out_copy(i):
        cols = aligned(i * (d // n_out), d // n_out)
        return pltpu.make_async_copy(ybuf.at[:, cols], y_hbm.at[:, cols], locs.at[MAX_LOCALS + i])

    def down(b, last=False):
        w_rows = aligned(b * blk, blk)

        @pl.loop(0, n_out)
        def _(i):
            cols = aligned(i * (d // n_out), d // n_out)
            total = hid[:, cols] + dot_nn(z[b], wdn[:, w_rows, cols].reshape(n_tp * blk, d // n_out))
            if last:
                ybuf[:, cols] = total.astype(BF16)
                out_copy(i).start()
            else:
                hid[:, cols] = total

    @pl.loop(0, n_chunk)
    def _(ch):
        attend(ch)

        @pl.when(ch < 2)
        def _():
            y_own(("a", ch), o_view(ch))

        @pl.when(ch == 1)
        def _():
            x_relay("o", out_view)

    l_kn = local(qkv.at[pl.ds(he, he)], kn_hbm)
    l_vn = local(qkv.at[pl.ds(2 * he, he)], vn_hbm)
    y_relay(("a", 0), o_view(0))
    y_own(("a", 2), o_view(2))
    x_relay("u", up_view)
    y_fin("dya", dny_view(0))
    y_fin("dyb", dny_view(1))
    x_own(("d", 0), dn_view(0))
    x_own(("d", 1), dn_view(1))
    y_relay(("a", 1), o_view(1))
    y_own(("a", 3), o_view(3))
    x_fin("o", out_view)
    y_relay(("a", 2), o_view(2))
    x_sib("o", out_view)

    @pl.loop(0, n_tok // PAIR)
    def _(p):
        for i in range(2):
            y_fin(("a", 2 * p + i), o_view(2 * p + i))
        project(p)

        @pl.when(p == 0)
        def _():
            x_fin("u", up_view)
            y_relay(("a", 3), o_view(3))
            y_own(("v", 0), ub_view(0))
            y_relay("u0", u0_view, True)
            y_own(("v", 1), ub_view(1))
            x_sib("u", up_view)

        up_own(p)

        @pl.when(p == 0)
        def _():
            x_relay(("d", 0), dn_view(0))
            x_own(("d", 2), dn_view(2))

    y_sib_near("u0", u0_view)
    y_relay(("v", 0), ub_view(0), True)
    y_own(("v", 2), ub_view(2))
    x_relay(("d", 1), dn_view(1))
    x_own(("d", 3), dn_view(3))
    y_fin("u0", u0_view, True)

    @pl.loop(0, BLOCKS)
    def _(b):
        y_sib_near(("v", b), ub_view(b))
        up_near(b)

        @pl.when(b == 0)
        def _():
            y_sib_far("u0", u0_view)

        @pl.when(b > 0)
        def _():
            y_sib_far(("v", b - 1), ub_view(b - 1))
            up_far(b - 1)

        @pl.when(b < BLOCKS - 1)
        def _():
            y_relay(("v", b + 1), ub_view(b + 1), True)

        @pl.when(b == 0)
        def _():
            y_own(("v", 3), ub_view(3))

        x_fin(("d", b), dn_view(b))

        @pl.when((b > 0) & (b < BLOCKS - 1))
        def _():
            x_relay(("d", b + 1), dn_view(b + 1))

        @pl.when(b == BLOCKS - 1)
        def _():
            y_fin(("v", b), ub_view(b), True)

        @pl.when(b > 0)
        def _():
            x_sib(("d", b - 1), dn_view(b - 1))
            down(b - 1)

        @pl.when(b < BLOCKS - 1)
        def _():
            y_fin(("v", b), ub_view(b), True)

    sent("g", "f", gbuf.at[pl.ds(0, 2 * n_x - 1)])
    for t, view in (("qa", qa_view), ("qb", qb_view), ("o", out_view), ("u", up_view)):
        x_sent(t, view)
    for t, view, share in (("oy", outy_view, False), ("dya", dny_view(0), False), ("dyb", dny_view(1), False), ("u0", u0_view, True)):
        y_sent(t, view, share)
    for b in range(BLOCKS):
        y_sent(("a", b), o_view(b))
        y_sent(("v", b), ub_view(b), True)
        x_sent(("d", b), dn_view(b))
    for copy in (l_kn, l_vn):
        copy.wait()
    x_sib(("d", BLOCKS - 1), dn_view(BLOCKS - 1))
    y_sib_far(("v", BLOCKS - 1), ub_view(BLOCKS - 1))
    up_far(BLOCKS - 1)
    down(BLOCKS - 1, True)
    for i in range(n_out):
        out_copy(i).wait()
    assert FAMILY_TENSORS + len(tensors) == TENSORS, len(tensors)
    assert FAMILY_ARRIVALS + len(arrivals) == ARRIVALS, len(arrivals)
    assert n_local[0] == MAX_LOCALS, n_local


def write_kernel(parts, *refs):
    n = (len(refs) - 1) // 3
    sems = refs[-1]
    moves = []
    for src, dst, buf in zip(refs[:n], refs[n:2 * n], refs[2 * n:3 * n]):
        rows = src.shape[0] // parts
        for i in range(parts):
            r = pl.ds(i * rows, rows)
            take = pltpu.make_async_copy(src.at[r], buf.at[r], sems.at[2 * len(moves)])
            take.start()
            moves.append((take, pltpu.make_async_copy(buf.at[r], dst.at[r], sems.at[2 * len(moves) + 1])))
    for take, put in moves:
        take.wait()
        put.start()
    for _, put in moves:
        put.wait()


def solution(mesh):
    tok_axes = ("dp", "wg")
    in_specs = (P(tok_axes, None), P("wg"), P("wg"), P("wg", None, "tp", None), P("wg", "tp", None), P("tp", None, "wg"), P("wg", "tp"), P("tp", "wg"), P("tp", None), P("tp", None), P(None, None), P(tok_axes, "tp", None, None), P(tok_axes, "tp", None, None), P(tok_axes))
    out_specs = (P(tok_axes, None), P(tok_axes, "tp", None), P(tok_axes, "tp", None))
    n_wg, n_tp = mesh.shape["wg"], mesh.shape["tp"]

    def device_step(tokens, gain_attn, gain_mlp, w_qkv, w_rel, w_out, w_up, w_down, bias_u, bias_v, rel_table, k_cache, v_cache, positions):
        n_tok, d = tokens.shape
        _, heads, slots, e_dim = k_cache.shape
        he = heads * e_dim
        piece, f_loc = w_up.shape
        w_q = jnp.transpose(w_qkv, (1, 2, 3, 0)).reshape(3 * he, piece)
        w_r = jnp.transpose(w_rel, (1, 2, 0)).reshape(he, piece)
        w_o = w_out.reshape(he, piece)
        k_t = jnp.transpose(k_cache, (1, 2, 3, 0))
        v_t = jnp.transpose(v_cache, (1, 2, 3, 0))
        hbm = pl.BlockSpec(memory_space=pl.ANY)
        vmem = pl.BlockSpec(memory_space=pltpu.VMEM)
        y, k_new, v_new = pl.pallas_call(
            functools.partial(layer_kernel, n_wg, n_tp, (heads, slots, e_dim)),
            out_shape=(jax.ShapeDtypeStruct((n_tok, d), BF16), jax.ShapeDtypeStruct((he, n_tok), BF16), jax.ShapeDtypeStruct((he, n_tok), BF16)),
            in_specs=[hbm] * 8 + [vmem] * 3 + [hbm] * 2 + [vmem],
            out_specs=(hbm, hbm, hbm),
            scratch_shapes=[
                pltpu.VMEM((n_tok, d), BF16),
                pltpu.VMEM(k_t.shape, BF16),
                pltpu.VMEM(v_t.shape, BF16),
                pltpu.VMEM((n_wg, 2, piece), F32),
                pltpu.VMEM((4 * he, d), BF16),
                pltpu.VMEM((n_tp * he, d), BF16),
                pltpu.VMEM((n_tp, n_wg // CORES, CORES, piece, f_loc), BF16),
                pltpu.VMEM((n_tp, f_loc, d), BF16),
                pltpu.VMEM((n_tok, d), BF16),
                pltpu.VMEM((3 * he, n_tok), BF16),
                pltpu.VMEM((he, CHUNK), BF16),
                pltpu.VMEM((slots * heads * slots, he), BF16),
                pltpu.VMEM((heads * slots, CHUNK), F32),
                pltpu.VMEM((n_tok, n_tp * he), BF16),
                pltpu.VMEM((he, CHUNK), F32),
                pltpu.VMEM((n_tok, d), F32),
                pltpu.VMEM((BLOCKS, n_tok, n_tp * (f_loc // BLOCKS)), BF16),
                pltpu.VMEM((n_tok, d), BF16),
                pltpu.SemaphoreType.DMA((TENSORS,)),
                pltpu.SemaphoreType.DMA((ARRIVALS,)),
                pltpu.SemaphoreType.DMA((MAX_LOCALS + 4,)),
            ],
            compiler_params=pltpu.CompilerParams(collective_id=0, has_side_effects=True, vmem_limit_bytes=67043328),
            name="decoder_layer",
        )(tokens, gain_attn.reshape(1, piece), gain_mlp.reshape(1, piece), w_q, w_r, w_o, w_up, w_down, bias_u, bias_v, rel_table, k_t, v_t, positions.reshape(1, n_tok))
        results = (y, k_new, v_new)
        y, k_new, v_new = pl.pallas_call(
            functools.partial(write_kernel, PARTS),
            out_shape=tuple(jax.ShapeDtypeStruct(r.shape, r.dtype) for r in results),
            in_specs=[hbm] * len(results),
            out_specs=(hbm,) * len(results),
            scratch_shapes=[pltpu.VMEM(r.shape, r.dtype) for r in results] + [pltpu.SemaphoreType.DMA((2 * PARTS * len(results),))],
            name="write_results",
        )(*results)
        k_new = jnp.transpose(k_new.reshape(heads, e_dim, n_tok), (2, 0, 1))
        v_new = jnp.transpose(v_new.reshape(heads, e_dim, n_tok), (2, 0, 1))
        return y, k_new, v_new

    return jax.shard_map(device_step, mesh=mesh, in_specs=in_specs, out_specs=out_specs, check_vma=False)
```

```python
import functools
import math

import jax
import jax.numpy as jnp
from jax import lax
from jax.experimental import pallas as pl
from jax.experimental.pallas import tpu as pltpu
from jax.sharding import PartitionSpec as P

NORM_EPS = 1e-6
GELU_A = (2.0 / math.pi) ** 0.5
GELU_B = 0.044715 * GELU_A
CORES = 2
CHUNK = 256
PAIR = 2 * CHUNK
BLOCKS = 4
PARTS = 4
FAMILY_TENSORS, FAMILY_ARRIVALS = 12, 48
TENSORS, ARRIVALS = 21, 80
MAX_LOCALS = 16
F32, BF16 = jnp.float32, jnp.bfloat16


def dot_nn(a, b):
    return lax.dot_general(a, b, (((1,), (0,)), ((), ())), preferred_element_type=F32)


def dot_nt(a, b):
    return lax.dot_general(a, b, (((1,), (1,)), ((), ())), preferred_element_type=F32)


def aligned(start, size):
    return pl.ds(pl.multiple_of(start, size), size)


def layer_kernel(n_wg, n_tp, dims, tok_hbm, ga_hbm, gm_hbm, wq_hbm, wr_hbm, wo_hbm, wu_hbm, wd_hbm, bu_hbm, bv_hbm, rt_hbm, kc_hbm, vc_hbm, pos_hbm,
                 y_hbm, kn_hbm, vn_hbm,
                 bu_ref, bv_ref, rt_ref, pos_ref, tok, kc, vc, gbuf, wqr, wout, wup, wdn, normed, qkv, rel, relp, rels, obuf, otr, hid, z, ybuf, sends, recvs, locs):
    heads, slots, e_dim = dims
    n_tok, d = tok.shape
    he = heads * e_dim
    f_loc = wu_hbm.shape[1]
    piece = d // n_wg
    n_x = n_wg // CORES
    n_chunk = n_tok // CHUNK
    blk = f_loc // BLOCKS
    wide = CORES * piece
    me = lax.axis_index("wg")
    x, c = me // CORES, lax.rem(me, CORES)
    y = lax.axis_index("tp")

    def at_x(off):
        return lax.rem(x + off + 2 * n_x, n_x)

    def wg_of(off, core):
        return at_x(off) * CORES + core

    def at_y(off):
        return lax.rem(y + off + n_tp, n_tp)

    other = 1 - c
    dev = {"x+": {"wg": wg_of(1, c)}, "x-": {"wg": wg_of(-1, c)}, "xx": {"wg": wg_of(2, c)}, "sib": {"wg": x * CORES + other}, "y+": {"tp": at_y(1)}, "y-": {"tp": at_y(-1)}}

    families = {"a": (0, 0, ("r", "l", "f")), "v": (4, 12, ("r", "l", "f", "n", "s")), "d": (8, 32, ("r", "l", "f", "s"))}
    tensors, arrivals = {}, {}

    def sem_ids(t, msg):
        if isinstance(t, tuple):
            tensor, base, msgs = families[t[0]]
            return tensor + t[1], base + t[1] * len(msgs) + msgs.index(msg)
        return FAMILY_TENSORS + tensors.setdefault(t, len(tensors)), FAMILY_ARRIVALS + arrivals.setdefault((t, msg), len(arrivals))

    def remote(t, msg, view, to, dst=None):
        i, k = sem_ids(t, msg)
        return pltpu.make_async_remote_copy(src_ref=view, dst_ref=view if dst is None else dst, send_sem=sends.at[i], recv_sem=recvs.at[k], device_id=dev[to], device_id_type=pl.DeviceIdType.MESH)

    def send(t, msg, view, to, dst=None):
        remote(t, msg, view, to, dst).start()

    def recv(t, msg, view):
        remote(t, msg, view, "sib").wait_recv()

    def sent(t, msg, view):
        remote(t, msg, view, "sib").wait_send()

    n_local = [0]

    def local(src, dst):
        copy = pltpu.make_async_copy(src, dst, locs.at[n_local[0]])
        n_local[0] += 1
        copy.start()
        return copy

    def x_own(t, view):
        v = view(0, c, None)
        send(t, "r", v, "x+", view(0, c, None, 1))
        send(t, "l", v, "x-", view(0, c, None, -1))
        send(t, "s", v, "sib")

    def x_relay(t, view):
        recv(t, "r", view(-1, c, None))
        send(t, "f", view(-1, c, 0), "x+", view(-1, c, 0, 1))
        recv(t, "l", view(1, c, None))
        send(t, "f", view(1, c, 1), "x-", view(1, c, 1, -1))
        send(t, "s", view(-1, c, None), "sib")
        send(t, "s", view(1, c, None), "sib")

    def x_fin(t, view):
        recv(t, "f", view(2, c, None))
        send(t, "s", view(2, c, None), "sib")

    def x_sib(t, view):
        recv(t, "s", view.many(n_x))

    def x_sent(t, view):
        sent(t, "r", view.many(n_x + 3))

    def y_own(t, view):
        v = view(0, None, c)
        send(t, "r", v, "y+", view(0, None, c, 1))
        send(t, "l", v, "y-", view(0, None, c, -1))

    def y_relay(t, view, share=False):
        recv(t, "r", view(-1, None, c))
        send(t, "f", view(-1, 0, c), "y+", view(-1, 0, c, 1))
        recv(t, "l", view(1, None, c))
        send(t, "f", view(1, 1, c), "y-", view(1, 1, c, -1))
        if share:
            send(t, "n", view(-1, None, c), "sib")
            send(t, "n", view(1, None, c), "sib")

    def y_fin(t, view, share=False):
        recv(t, "f", view(2, None, c))
        if share:
            send(t, "s", view(2, None, c), "sib")

    def y_sib_near(t, view):
        recv(t, "n", view.many(2))

    def y_sib_far(t, view):
        recv(t, "s", view(2, None, other))

    def y_sent(t, view, share=False):
        sent(t, "r", view.many(6 if share else 3))

    def sized(view, many):
        view.many = many
        return view

    def rows_of(start, size, half):
        if half is None:
            return aligned(start, size)
        return aligned(start + half * (size // 2), size // 2)

    def col_view(ref, row0, n_rows):
        def view(off, core, half, hop=0):
            return ref.at[rows_of(row0, n_rows, half), aligned(wg_of(off, core) * piece, piece)]
        return sized(view, lambda n: ref.at[pl.ds(row0, n_rows), pl.ds(0, n * piece)])

    half_q = wqr.shape[0] // 2
    qa_view = col_view(wqr, 0, half_q)
    qb_view = col_view(wqr, half_q, half_q)
    out_view = col_view(wout, 0, wout.shape[0])

    def outy_view(off, half, core, hop=0):
        return wout.at[rows_of(at_y(off) * he, he, half), aligned(wg_of(0, core) * piece, piece)]

    sized(outy_view, lambda n: wout.at[pl.ds(0, n * he), pl.ds(0, piece)])

    def slot(off):
        return (off + 1) % n_tp

    def dny_view(part):
        rows = f_loc // 2

        def view(off, half, core, hop=0):
            return wdn.at[slot(off - hop), rows_of(part * rows, rows, half), aligned(wg_of(0, core) * piece, piece)]
        return sized(view, lambda n: wdn.at[pl.ds(0, n), pl.ds(part * rows, rows), pl.ds(0, piece)])

    def dn_view(b):
        def view(off, core, half, hop=0):
            return wdn.at[:, rows_of(b * blk, blk, half), aligned(wg_of(off, core) * piece, piece)]
        return sized(view, lambda n: wdn.at[:, aligned(b * blk, blk), pl.ds(0, n * piece)])

    def up_view(off, core, half, hop=0):
        return wup.at[y, (off - hop) % n_x, core, rows_of(0, piece, half)]

    sized(up_view, lambda n: wup.at[y, :, :, :, pl.ds(0, n * f_loc // n_wg)])

    def u0_view(off, half, core, hop=0):
        return wup.at[at_y(off), 0, core, rows_of(0, piece, half)]

    sized(u0_view, lambda n: wup.at[pl.ds(0, n // CORES), 0])

    def ub_view(b):
        def view(off, half, core, hop=0):
            return wup.at[at_y(off), pl.ds(1, n_x - 1), core, rows_of(0, piece, half), aligned(b * blk, blk)]
        return sized(view, lambda n: wup.at[pl.ds(0, n // CORES), pl.ds(1, n_x - 1), :, :, aligned(b * blk, blk)])

    def o_view(ch):
        def view(off, half, core, hop=0):
            return obuf.at[rows_of(ch * CHUNK, CHUNK, half), aligned(at_y(off) * he, he)]
        return sized(view, lambda n: obuf.at[aligned(ch * CHUNK, CHUNK), pl.ds(0, n * he)])

    own_cols = aligned(me * piece, piece)
    n_qkv = wq_hbm.shape[0]
    l_g = [local(ga_hbm, gbuf.at[me, pl.ds(0, 1)]), local(gm_hbm, gbuf.at[me, pl.ds(1, 1)])]
    l_w = [local(wq_hbm, wqr.at[pl.ds(0, n_qkv), own_cols]), local(wr_hbm, wqr.at[pl.ds(n_qkv, he), own_cols])]
    l_o = local(wo_hbm, wout.at[aligned(y * he, he), own_cols])
    l_t = local(tok_hbm, tok)
    l_d = local(wd_hbm, wdn.at[slot(0), :, own_cols])
    l_u = local(wu_hbm, wup.at[y, 0, c])
    l_s = [local(src, dst) for src, dst in ((bu_hbm, bu_ref), (bv_hbm, bv_ref), (rt_hbm, rt_ref), (pos_hbm, pos_ref))]
    l_k = local(kc_hbm, kc)
    l_v = local(vc_hbm, vc)

    barrier = pltpu.get_barrier_semaphore()
    for to in dev.values():
        pl.semaphore_signal(barrier, inc=1, device_id=to, device_id_type=pl.DeviceIdType.MESH)
    pl.semaphore_wait(barrier, len(dev))

    for copy in l_g:
        copy.wait()
    for to in ("x+", "x-", "xx"):
        send("g", "f", gbuf.at[me], to)
    send("g", "s", gbuf.at[me], "sib")
    for copy in l_w:
        copy.wait()
    x_own("qa", qa_view)
    x_own("qb", qb_view)
    l_o.wait()
    y_own("oy", outy_view)
    l_d.wait()
    y_own("dya", dny_view(0))
    recv("g", "f", gbuf.at[pl.ds(0, n_x - 1)])
    for k in range(1, n_x):
        send("g", "s", gbuf.at[wg_of(k, c)], "sib")
    y_relay("oy", outy_view)
    y_own("dyb", dny_view(1))
    l_u.wait()
    y_own("u0", u0_view)
    x_relay("qa", qa_view)
    recv("g", "s", gbuf.at[pl.ds(0, n_x)])
    l_t.wait()

    def gain_row(i):
        return jnp.concatenate([gbuf[w, i:i + 1, :] for w in range(n_wg)], axis=1)

    def norm(vals, gain):
        mean_sq = jnp.mean(vals * vals, axis=-1, keepdims=True)
        return (vals * lax.rsqrt(mean_sq + NORM_EPS) * gain).astype(BF16)

    norm_rows = 64

    @pl.loop(0, n_tok // norm_rows)
    def _(i):
        r = aligned(i * norm_rows, norm_rows)
        normed[r, :] = norm(tok[r, :].astype(F32), gain_row(0))

    x_relay("qb", qb_view)
    y_fin("oy", outy_view)
    x_own("o", out_view)
    x_own("u", up_view)
    x_fin("qa", qa_view)
    x_fin("qb", qb_view)
    y_relay("dya", dny_view(0))
    y_relay("dyb", dny_view(1))
    x_sib("qa", qa_view)
    x_sib("qb", qb_view)

    for copy in l_s:
        copy.wait()

    n_rel = slots * heads * slots
    row = lax.broadcasted_iota(jnp.int32, (n_rel, slots), 0)
    col = lax.broadcasted_iota(jnp.int32, (n_rel, slots), 1)
    offset = jnp.maximum(row // (heads * slots) - lax.rem(row, slots), 0)
    pick = jnp.where(col == offset, 1.0, 0.0).astype(BF16)
    table = dot_nn(pick, rt_ref[...]).astype(BF16)
    rel_q = dot_nt(table, wqr[n_qkv:n_qkv + he, :]).astype(BF16).astype(F32)
    row = lax.broadcasted_iota(jnp.int32, (n_rel, he), 0)
    col = lax.broadcasted_iota(jnp.int32, (n_rel, he), 1)
    relp[...] = jnp.where(lax.rem(row // slots, heads) == col // e_dim, rel_q, 0.0).astype(BF16)

    eye = lax.broadcasted_iota(jnp.int32, (e_dim, e_dim), 0) == lax.broadcasted_iota(jnp.int32, (e_dim, e_dim), 1)

    def bias_col(ref, h):
        return jnp.sum(jnp.where(eye, ref[h:h + 1, :], 0.0), axis=1, keepdims=True)

    l_k.wait()
    l_v.wait()
    scale = e_dim ** -0.5

    def attend(ch):
        cols = aligned(ch * CHUNK, CHUNK)
        pos = pos_ref[:, cols]
        chunk = normed[cols, :]
        qkv[:, cols] = dot_nt(wqr[0:n_qkv, :], chunk).astype(BF16)
        for h in range(heads):
            q = qkv[h * e_dim:(h + 1) * e_dim, cols].astype(F32)
            rel[h * e_dim:(h + 1) * e_dim, :] = (q + bias_col(bv_ref, h)).astype(BF16)
            otr[h * e_dim:(h + 1) * e_dim, :] = (q + bias_col(bu_ref, h)).astype(BF16).astype(F32)
        rel_all = dot_nn(relp[...], rel[...])
        per_p = heads * slots
        sel = jnp.zeros((per_p, CHUNK), F32)
        for p in range(slots):
            sel = jnp.where(pos == p, rel_all[p * per_p:(p + 1) * per_p, :], sel)
        rels[...] = sel

        @pl.loop(0, heads)
        def _(h):
            r = aligned(h * e_dim, e_dim)
            qu = otr[r, :]
            k_new = qkv[aligned(he + h * e_dim, e_dim), cols].astype(F32)
            v_new = qkv[aligned(2 * he + h * e_dim, e_dim), cols].astype(F32)
            rel_h = rels[aligned(h * slots, slots), :]
            self_s = jnp.sum(qu * k_new, axis=0, keepdims=True)
            scores = []
            for j in range(slots):
                s = jnp.sum(qu * kc[h, j, :, cols].astype(F32), axis=0, keepdims=True)
                s = (jnp.where(pos == j, self_s, s) + rel_h[j:j + 1, :]) * scale
                scores.append(jnp.where(pos >= j, s, -1e30))
            top = functools.reduce(jnp.maximum, scores)
            exps = [jnp.exp(s - top) for s in scores]
            total = functools.reduce(jnp.add, exps)
            self_a = jnp.zeros_like(total)
            out = jnp.zeros((e_dim, CHUNK), F32)
            for j in range(slots):
                a = (exps[j] / total).astype(BF16).astype(F32)
                self_a = jnp.where(pos == j, a, self_a)
                out = out + jnp.where(pos > j, a, 0.0) * vc[h, j, :, cols].astype(F32)
            otr[r, :] = out + self_a * v_new

        obuf[cols, aligned(y * he, he)] = otr[...].T.astype(BF16)

    def project(pair):
        r = aligned(pair * PAIR, PAIR)
        hid[r, :] = tok[r, :].astype(F32) + dot_nn(obuf[r, :], wout[...])
        gain = gain_row(1)

        @pl.loop(0, PAIR // norm_rows)
        def _(i):
            q = aligned(pair * PAIR + i * norm_rows, norm_rows)
            m = norm(hid[q, :], gain)
            for k in range(n_x):
                normed[q, aligned(lax.rem(k - x + n_x, n_x) * wide, wide)] = m[:, k * wide:(k + 1) * wide]

    def gelu(v):
        half = 0.5 * v
        return half + half * jnp.tanh(v * (GELU_A + GELU_B * (v * v)))

    def up_rows(r, off, b):
        cols = aligned(b * blk, blk)
        w = wup[at_y(off), :, :, :, cols].reshape(d, blk)
        z[b, r, pl.ds(slot(off) * blk, blk)] = gelu(dot_nn(normed[r, :], w)).astype(BF16)

    def up_own(pair):
        @pl.loop(0, BLOCKS // 2)
        def _(i):
            for k in range(2):
                up_rows(aligned(pair * PAIR, PAIR), 0, 2 * i + k)

    def up_near(b, between=None):
        @pl.loop(0, n_tok // PAIR)
        def _(i):
            for off in (-1, 1):
                up_rows(aligned(i * PAIR, PAIR), off, b)
            if between is not None:
                pl.when(i == 0)(between)

    def down_rows(r, b, first, count):
        w = wdn[first:first + count, aligned(b * blk, blk), :].reshape(count * blk, d)
        hid[r, :] += dot_nn(z[b, r, first * blk:(first + count) * blk], w)

    def down_near(b):
        @pl.loop(0, n_tok // PAIR)
        def _(i):
            down_rows(aligned(i * PAIR, PAIR), b, 0, n_tp - 1)

    def far_down(b, first, between=None):
        @pl.loop(0, n_tok // PAIR)
        def _(i):
            r = aligned(i * PAIR, PAIR)
            up_rows(r, 2, b)
            down_rows(r, b, first, n_tp - first)
            if between is not None:
                pl.when(i == 0)(between)

    n_out = 4

    def out_copy(i):
        cols = aligned(i * (d // n_out), d // n_out)
        return pltpu.make_async_copy(ybuf.at[:, cols], y_hbm.at[:, cols], locs.at[MAX_LOCALS + i])

    def last_block(b):
        up_rows(slice(None), 2, b)
        for i in range(n_out):
            cols = pl.ds(i * (d // n_out), d // n_out)
            w = wdn[:, b * blk:(b + 1) * blk, cols].reshape(n_tp * blk, d // n_out)
            ybuf[:, cols] = (hid[:, cols] + dot_nn(z[b], w)).astype(BF16)
            out_copy(i).start()

    @pl.loop(0, n_chunk)
    def _(ch):
        attend(ch)

        @pl.when(ch < 2)
        def _():
            y_own(("a", ch), o_view(ch))

        @pl.when(ch == 2)
        def _():
            x_relay("o", out_view)

    l_kn = local(qkv.at[pl.ds(he, he)], kn_hbm)
    l_vn = local(qkv.at[pl.ds(2 * he, he)], vn_hbm)
    y_relay(("a", 0), o_view(0))
    y_own(("a", 2), o_view(2))
    x_relay("u", up_view)
    y_fin("dya", dny_view(0))
    y_fin("dyb", dny_view(1))
    x_own(("d", 0), dn_view(0))
    x_own(("d", 1), dn_view(1))
    y_relay(("a", 1), o_view(1))
    y_own(("a", 3), o_view(3))
    x_fin("o", out_view)
    y_relay(("a", 2), o_view(2))
    y_relay("u0", u0_view, True)
    x_sib("o", out_view)

    @pl.loop(0, n_tok // PAIR)
    def _(p):
        for i in range(2):
            y_fin(("a", 2 * p + i), o_view(2 * p + i))
        project(p)

        @pl.when(p == 0)
        def _():
            x_fin("u", up_view)
            y_relay(("a", 3), o_view(3))
            y_own(("v", 0), ub_view(0))
            y_own(("v", 1), ub_view(1))
            x_sib("u", up_view)

        up_own(p)

        @pl.when(p == 0)
        def _():
            x_relay(("d", 0), dn_view(0))
            x_own(("d", 2), dn_view(2))

    y_sib_near("u0", u0_view)
    y_relay(("v", 0), ub_view(0), True)
    y_own(("v", 2), ub_view(2))
    x_relay(("d", 1), dn_view(1))
    x_own(("d", 3), dn_view(3))
    y_fin("u0", u0_view, True)
    x_fin(("d", 0), dn_view(0))
    y_sib_near(("v", 0), ub_view(0))
    up_near(0)
    y_relay(("v", 1), ub_view(1), True)
    y_own(("v", 3), ub_view(3))
    y_sib_far("u0", u0_view)
    x_sib(("d", 0), dn_view(0))
    down_near(0)

    @pl.loop(1, BLOCKS)
    def _(b):
        y_sib_near(("v", b), ub_view(b))
        up_near(b, lambda: y_fin(("v", b - 1), ub_view(b - 1), True))
        y_sib_far(("v", b - 1), ub_view(b - 1))

        @pl.when(b < BLOCKS - 1)
        def _():
            x_relay(("d", b + 1), dn_view(b + 1))

        def between():
            @pl.when(b < BLOCKS - 1)
            def _():
                y_relay(("v", b + 1), ub_view(b + 1), True)

            @pl.when(b == BLOCKS - 1)
            def _():
                y_fin(("v", b), ub_view(b), True)
                x_fin(("d", b), dn_view(b))

        @pl.when(b == 1)
        def _():
            far_down(0, n_tp - 1, between)

        @pl.when(b > 1)
        def _():
            x_sib(("d", b - 1), dn_view(b - 1))
            far_down(b - 1, 0, between)

        @pl.when(b < BLOCKS - 1)
        def _():
            x_fin(("d", b), dn_view(b))

    sent("g", "f", gbuf.at[pl.ds(0, 2 * n_x - 1)])
    for t, view in (("qa", qa_view), ("qb", qb_view), ("o", out_view), ("u", up_view)):
        x_sent(t, view)
    for t, view, share in (("oy", outy_view, False), ("dya", dny_view(0), False), ("dyb", dny_view(1), False), ("u0", u0_view, True)):
        y_sent(t, view, share)
    for b in range(BLOCKS):
        y_sent(("a", b), o_view(b))
        y_sent(("v", b), ub_view(b), True)
        x_sent(("d", b), dn_view(b))
    for copy in (l_kn, l_vn):
        copy.wait()
    x_sib(("d", BLOCKS - 1), dn_view(BLOCKS - 1))
    y_sib_far(("v", BLOCKS - 1), ub_view(BLOCKS - 1))
    last_block(BLOCKS - 1)
    for i in range(n_out):
        out_copy(i).wait()
    assert FAMILY_TENSORS + len(tensors) == TENSORS, len(tensors)
    assert FAMILY_ARRIVALS + len(arrivals) == ARRIVALS, len(arrivals)
    assert n_local[0] == MAX_LOCALS, n_local


def write_kernel(parts, *refs):
    n = (len(refs) - 1) // 3
    sems = refs[-1]
    moves = []
    for src, dst, buf in zip(refs[:n], refs[n:2 * n], refs[2 * n:3 * n]):
        rows = src.shape[0] // parts
        for i in range(parts):
            r = pl.ds(i * rows, rows)
            take = pltpu.make_async_copy(src.at[r], buf.at[r], sems.at[2 * len(moves)])
            take.start()
            moves.append((take, pltpu.make_async_copy(buf.at[r], dst.at[r], sems.at[2 * len(moves) + 1])))
    for take, put in moves:
        take.wait()
        put.start()
    for _, put in moves:
        put.wait()


def solution(mesh):
    tok_axes = ("dp", "wg")
    in_specs = (P(tok_axes, None), P("wg"), P("wg"), P("wg", None, "tp", None), P("wg", "tp", None), P("tp", None, "wg"), P("wg", "tp"), P("tp", "wg"), P("tp", None), P("tp", None), P(None, None), P(tok_axes, "tp", None, None), P(tok_axes, "tp", None, None), P(tok_axes))
    out_specs = (P(tok_axes, None), P(tok_axes, "tp", None), P(tok_axes, "tp", None))
    n_wg, n_tp = mesh.shape["wg"], mesh.shape["tp"]

    def device_step(tokens, gain_attn, gain_mlp, w_qkv, w_rel, w_out, w_up, w_down, bias_u, bias_v, rel_table, k_cache, v_cache, positions):
        n_tok, d = tokens.shape
        _, heads, slots, e_dim = k_cache.shape
        he = heads * e_dim
        piece, f_loc = w_up.shape
        w_q = jnp.transpose(w_qkv, (1, 2, 3, 0)).reshape(3 * he, piece)
        w_r = jnp.transpose(w_rel, (1, 2, 0)).reshape(he, piece)
        w_o = w_out.reshape(he, piece)
        k_t = jnp.transpose(k_cache, (1, 2, 3, 0))
        v_t = jnp.transpose(v_cache, (1, 2, 3, 0))
        hbm = pl.BlockSpec(memory_space=pl.ANY)
        y, k_new, v_new = pl.pallas_call(
            functools.partial(layer_kernel, n_wg, n_tp, (heads, slots, e_dim)),
            out_shape=(jax.ShapeDtypeStruct((n_tok, d), BF16), jax.ShapeDtypeStruct((he, n_tok), BF16), jax.ShapeDtypeStruct((he, n_tok), BF16)),
            in_specs=[hbm] * 14,
            out_specs=(hbm, hbm, hbm),
            scratch_shapes=[
                pltpu.VMEM(bias_u.shape, F32),
                pltpu.VMEM(bias_v.shape, F32),
                pltpu.VMEM(rel_table.shape, BF16),
                pltpu.VMEM((1, n_tok), jnp.int32),
                pltpu.VMEM((n_tok, d), BF16),
                pltpu.VMEM(k_t.shape, BF16),
                pltpu.VMEM(v_t.shape, BF16),
                pltpu.VMEM((n_wg, 2, piece), F32),
                pltpu.VMEM((4 * he, d), BF16),
                pltpu.VMEM((n_tp * he, d), BF16),
                pltpu.VMEM((n_tp, n_wg // CORES, CORES, piece, f_loc), BF16),
                pltpu.VMEM((n_tp, f_loc, d), BF16),
                pltpu.VMEM((n_tok, d), BF16),
                pltpu.VMEM((3 * he, n_tok), BF16),
                pltpu.VMEM((he, CHUNK), BF16),
                pltpu.VMEM((slots * heads * slots, he), BF16),
                pltpu.VMEM((heads * slots, CHUNK), F32),
                pltpu.VMEM((n_tok, n_tp * he), BF16),
                pltpu.VMEM((he, CHUNK), F32),
                pltpu.VMEM((n_tok, d), F32),
                pltpu.VMEM((BLOCKS, n_tok, n_tp * (f_loc // BLOCKS)), BF16),
                pltpu.VMEM((n_tok, d), BF16),
                pltpu.SemaphoreType.DMA((TENSORS,)),
                pltpu.SemaphoreType.DMA((ARRIVALS,)),
                pltpu.SemaphoreType.DMA((MAX_LOCALS + 4,)),
            ],
            compiler_params=pltpu.CompilerParams(collective_id=0, has_side_effects=True, vmem_limit_bytes=67043328),
            name="decoder_layer",
        )(tokens, gain_attn.reshape(1, piece), gain_mlp.reshape(1, piece), w_q, w_r, w_o, w_up, w_down, bias_u, bias_v, rel_table, k_t, v_t, positions.reshape(1, n_tok))
        results = (y, k_new, v_new)
        y, k_new, v_new = pl.pallas_call(
            functools.partial(write_kernel, PARTS),
            out_shape=tuple(jax.ShapeDtypeStruct(r.shape, r.dtype) for r in results),
            in_specs=[hbm] * len(results),
            out_specs=(hbm,) * len(results),
            scratch_shapes=[pltpu.VMEM(r.shape, r.dtype) for r in results] + [pltpu.SemaphoreType.DMA((2 * PARTS * len(results),))],
            name="write_results",
        )(*results)
        k_new = jnp.transpose(k_new.reshape(heads, e_dim, n_tok), (2, 0, 1))
        v_new = jnp.transpose(v_new.reshape(heads, e_dim, n_tok), (2, 0, 1))
        return y, k_new, v_new

    return jax.shard_map(device_step, mesh=mesh, in_specs=in_specs, out_specs=out_specs, check_vma=False)
```

```python
import functools
import math

import jax
import jax.numpy as jnp
from jax import lax
from jax.experimental import pallas as pl
from jax.experimental.pallas import tpu as pltpu
from jax.sharding import PartitionSpec as P

NORM_EPS = 1e-6
GELU_A = (2.0 / math.pi) ** 0.5
GELU_B = 0.044715 * GELU_A
CORES = 2
CHUNK = 256
PAIR = 2 * CHUNK
BLOCKS = 4
PARTS = 2
KERNEL_VMEM = 55574528
FAMILY_TENSORS, FAMILY_ARRIVALS = 12, 48
TENSORS, ARRIVALS = 21, 80
MAX_LOCALS = 14
F32, BF16 = jnp.float32, jnp.bfloat16


def dot_nn(a, b):
    return lax.dot_general(a, b, (((1,), (0,)), ((), ())), preferred_element_type=F32)


def dot_nt(a, b):
    return lax.dot_general(a, b, (((1,), (1,)), ((), ())), preferred_element_type=F32)


def aligned(start, size):
    return pl.ds(pl.multiple_of(start, size), size)


def layer_kernel(n_wg, n_tp, dims, tok_hbm, ga_hbm, gm_hbm, wq_hbm, wr_hbm, wo_hbm, wu_hbm, wd_hbm, bu_hbm, bv_hbm, rt_hbm, kc_hbm, vc_hbm, pos_hbm,
                 y_out, kn_out, vn_out,
                 bu_ref, bv_ref, rt_ref, pos_ref, tok, kc, vc, gbuf, wqr, wout, wup, wdn, normed, qkv, rel, relp, rels, obuf, otr, hid, z, sends, recvs, locs):
    heads, slots, e_dim = dims
    n_tok, d = tok.shape
    he = heads * e_dim
    f_loc = wu_hbm.shape[1]
    piece = d // n_wg
    n_x = n_wg // CORES
    n_chunk = n_tok // CHUNK
    blk = f_loc // BLOCKS
    wide = CORES * piece
    me = lax.axis_index("wg")
    x, c = me // CORES, lax.rem(me, CORES)
    y = lax.axis_index("tp")

    def at_x(off):
        return lax.rem(x + off + 2 * n_x, n_x)

    def wg_of(off, core):
        return at_x(off) * CORES + core

    def at_y(off):
        return lax.rem(y + off + n_tp, n_tp)

    other = 1 - c
    dev = {"x+": {"wg": wg_of(1, c)}, "x-": {"wg": wg_of(-1, c)}, "xx": {"wg": wg_of(2, c)}, "sib": {"wg": x * CORES + other}, "y+": {"tp": at_y(1)}, "y-": {"tp": at_y(-1)}}

    families = {"a": (0, 0, ("r", "l", "f")), "v": (4, 12, ("r", "l", "f", "n", "s")), "d": (8, 32, ("r", "l", "f", "s"))}
    tensors, arrivals = {}, {}

    def sem_ids(t, msg):
        if isinstance(t, tuple):
            tensor, base, msgs = families[t[0]]
            return tensor + t[1], base + t[1] * len(msgs) + msgs.index(msg)
        return FAMILY_TENSORS + tensors.setdefault(t, len(tensors)), FAMILY_ARRIVALS + arrivals.setdefault((t, msg), len(arrivals))

    def remote(t, msg, view, to, dst=None):
        i, k = sem_ids(t, msg)
        return pltpu.make_async_remote_copy(src_ref=view, dst_ref=view if dst is None else dst, send_sem=sends.at[i], recv_sem=recvs.at[k], device_id=dev[to], device_id_type=pl.DeviceIdType.MESH)

    def send(t, msg, view, to, dst=None):
        remote(t, msg, view, to, dst).start()

    def recv(t, msg, view):
        remote(t, msg, view, "sib").wait_recv()

    def sent(t, msg, view):
        remote(t, msg, view, "sib").wait_send()

    n_local = [0]

    def local(src, dst):
        copy = pltpu.make_async_copy(src, dst, locs.at[n_local[0]])
        n_local[0] += 1
        copy.start()
        return copy

    def x_own(t, view):
        v = view(0, c, None)
        send(t, "r", v, "x+", view(0, c, None, 1))
        send(t, "l", v, "x-", view(0, c, None, -1))
        send(t, "s", v, "sib")

    def x_relay(t, view):
        recv(t, "r", view(-1, c, None))
        send(t, "f", view(-1, c, 0), "x+", view(-1, c, 0, 1))
        recv(t, "l", view(1, c, None))
        send(t, "f", view(1, c, 1), "x-", view(1, c, 1, -1))
        send(t, "s", view(-1, c, None), "sib")
        send(t, "s", view(1, c, None), "sib")

    def x_fin(t, view):
        recv(t, "f", view(2, c, None))
        send(t, "s", view(2, c, None), "sib")

    def x_sib(t, view):
        recv(t, "s", view.many(n_x))

    def x_sent(t, view):
        sent(t, "r", view.many(n_x + 3))

    def y_own(t, view):
        v = view(0, None, c)
        send(t, "r", v, "y+", view(0, None, c, 1))
        send(t, "l", v, "y-", view(0, None, c, -1))

    def y_relay(t, view, share=False):
        recv(t, "r", view(-1, None, c))
        send(t, "f", view(-1, 0, c), "y+", view(-1, 0, c, 1))
        recv(t, "l", view(1, None, c))
        send(t, "f", view(1, 1, c), "y-", view(1, 1, c, -1))
        if share:
            send(t, "n", view(-1, None, c), "sib")
            send(t, "n", view(1, None, c), "sib")

    def y_fin(t, view, share=False):
        recv(t, "f", view(2, None, c))
        if share:
            send(t, "s", view(2, None, c), "sib")

    def y_sib_near(t, view):
        recv(t, "n", view.many(2))

    def y_sib_far(t, view):
        recv(t, "s", view(2, None, other))

    def y_sent(t, view, share=False):
        sent(t, "r", view.many(6 if share else 3))

    def sized(view, many):
        view.many = many
        return view

    def rows_of(start, size, half):
        if half is None:
            return aligned(start, size)
        return aligned(start + half * (size // 2), size // 2)

    def col_view(ref, row0, n_rows):
        def view(off, core, half, hop=0):
            return ref.at[rows_of(row0, n_rows, half), aligned(wg_of(off, core) * piece, piece)]
        return sized(view, lambda n: ref.at[pl.ds(row0, n_rows), pl.ds(0, n * piece)])

    half_q = wqr.shape[0] // 2
    qa_view = col_view(wqr, 0, half_q)
    qb_view = col_view(wqr, half_q, half_q)
    out_view = col_view(wout, 0, wout.shape[0])

    def outy_view(off, half, core, hop=0):
        return wout.at[rows_of(at_y(off) * he, he, half), aligned(wg_of(0, core) * piece, piece)]

    sized(outy_view, lambda n: wout.at[pl.ds(0, n * he), pl.ds(0, piece)])

    def slot(off):
        return (off + 1) % n_tp

    def dny_view(part):
        rows = f_loc // 2

        def view(off, half, core, hop=0):
            return wdn.at[slot(off - hop), rows_of(part * rows, rows, half), aligned(wg_of(0, core) * piece, piece)]
        return sized(view, lambda n: wdn.at[pl.ds(0, n), pl.ds(part * rows, rows), pl.ds(0, piece)])

    def dn_view(b):
        def view(off, core, half, hop=0):
            return wdn.at[:, rows_of(b * blk, blk, half), aligned(wg_of(off, core) * piece, piece)]
        return sized(view, lambda n: wdn.at[:, aligned(b * blk, blk), pl.ds(0, n * piece)])

    def up_view(off, core, half, hop=0):
        return wup.at[y, (off - hop) % n_x, core, rows_of(0, piece, half)]

    sized(up_view, lambda n: wup.at[y, :, :, :, pl.ds(0, n * f_loc // n_wg)])

    def u0_view(off, half, core, hop=0):
        return wup.at[at_y(off), 0, core, rows_of(0, piece, half)]

    sized(u0_view, lambda n: wup.at[pl.ds(0, n // CORES), 0])

    def ub_view(b):
        def view(off, half, core, hop=0):
            return wup.at[at_y(off), pl.ds(1, n_x - 1), core, rows_of(0, piece, half), aligned(b * blk, blk)]
        return sized(view, lambda n: wup.at[pl.ds(0, n // CORES), pl.ds(1, n_x - 1), :, :, aligned(b * blk, blk)])

    def o_view(ch):
        def view(off, half, core, hop=0):
            return obuf.at[rows_of(ch * CHUNK, CHUNK, half), aligned(at_y(off) * he, he)]
        return sized(view, lambda n: obuf.at[aligned(ch * CHUNK, CHUNK), pl.ds(0, n * he)])

    own_cols = aligned(me * piece, piece)
    n_qkv = wq_hbm.shape[0]
    l_g = [local(ga_hbm, gbuf.at[me, pl.ds(0, 1)]), local(gm_hbm, gbuf.at[me, pl.ds(1, 1)])]
    l_w = [local(wq_hbm, wqr.at[pl.ds(0, n_qkv), own_cols]), local(wr_hbm, wqr.at[pl.ds(n_qkv, he), own_cols])]
    l_o = local(wo_hbm, wout.at[aligned(y * he, he), own_cols])
    l_t = local(tok_hbm, tok)
    l_d = local(wd_hbm, wdn.at[slot(0), :, own_cols])
    l_u = local(wu_hbm, wup.at[y, 0, c])
    l_s = [local(src, dst) for src, dst in ((bu_hbm, bu_ref), (bv_hbm, bv_ref), (rt_hbm, rt_ref), (pos_hbm, pos_ref))]
    l_k = local(kc_hbm, kc)
    l_v = local(vc_hbm, vc)

    barrier = pltpu.get_barrier_semaphore()
    for to in dev.values():
        pl.semaphore_signal(barrier, inc=1, device_id=to, device_id_type=pl.DeviceIdType.MESH)
    pl.semaphore_wait(barrier, len(dev))

    for copy in l_g:
        copy.wait()
    for to in ("x+", "x-", "xx"):
        send("g", "f", gbuf.at[me], to)
    send("g", "s", gbuf.at[me], "sib")
    for copy in l_w:
        copy.wait()
    x_own("qa", qa_view)
    x_own("qb", qb_view)
    l_o.wait()
    y_own("oy", outy_view)
    l_d.wait()
    y_own("dya", dny_view(0))
    recv("g", "f", gbuf.at[pl.ds(0, n_x - 1)])
    for k in range(1, n_x):
        send("g", "s", gbuf.at[wg_of(k, c)], "sib")
    y_relay("oy", outy_view)
    y_own("dyb", dny_view(1))
    l_u.wait()
    y_own("u0", u0_view)
    x_relay("qa", qa_view)
    recv("g", "s", gbuf.at[pl.ds(0, n_x)])
    l_t.wait()

    def gain_row(i):
        return jnp.concatenate([gbuf[w, i:i + 1, :] for w in range(n_wg)], axis=1)

    def norm(vals, gain):
        mean_sq = jnp.mean(vals * vals, axis=-1, keepdims=True)
        return (vals * lax.rsqrt(mean_sq + NORM_EPS) * gain).astype(BF16)

    norm_rows = 64

    @pl.loop(0, n_tok // norm_rows)
    def _(i):
        r = aligned(i * norm_rows, norm_rows)
        normed[r, :] = norm(tok[r, :].astype(F32), gain_row(0))

    x_relay("qb", qb_view)
    y_fin("oy", outy_view)
    x_own("o", out_view)
    x_own("u", up_view)
    x_fin("qa", qa_view)
    x_fin("qb", qb_view)
    y_relay("dya", dny_view(0))
    y_relay("dyb", dny_view(1))
    x_sib("qa", qa_view)
    x_sib("qb", qb_view)

    for copy in l_s:
        copy.wait()

    n_rel = slots * heads * slots
    row = lax.broadcasted_iota(jnp.int32, (n_rel, slots), 0)
    col = lax.broadcasted_iota(jnp.int32, (n_rel, slots), 1)
    offset = jnp.maximum(row // (heads * slots) - lax.rem(row, slots), 0)
    pick = jnp.where(col == offset, 1.0, 0.0).astype(BF16)
    table = dot_nn(pick, rt_ref[...]).astype(BF16)
    rel_q = dot_nt(table, wqr[n_qkv:n_qkv + he, :]).astype(BF16).astype(F32)
    row = lax.broadcasted_iota(jnp.int32, (n_rel, he), 0)
    col = lax.broadcasted_iota(jnp.int32, (n_rel, he), 1)
    relp[...] = jnp.where(lax.rem(row // slots, heads) == col // e_dim, rel_q, 0.0).astype(BF16)

    eye = lax.broadcasted_iota(jnp.int32, (e_dim, e_dim), 0) == lax.broadcasted_iota(jnp.int32, (e_dim, e_dim), 1)

    def bias_col(ref, h):
        return jnp.sum(jnp.where(eye, ref[h:h + 1, :], 0.0), axis=1, keepdims=True)

    l_k.wait()
    l_v.wait()
    scale = e_dim ** -0.5

    def attend(ch):
        cols = aligned(ch * CHUNK, CHUNK)
        pos = pos_ref[:, cols]
        chunk = normed[cols, :]
        qkv[:, cols] = dot_nt(wqr[0:n_qkv, :], chunk).astype(BF16)
        for h in range(heads):
            q = qkv[h * e_dim:(h + 1) * e_dim, cols].astype(F32)
            rel[h * e_dim:(h + 1) * e_dim, :] = (q + bias_col(bv_ref, h)).astype(BF16)
            otr[h * e_dim:(h + 1) * e_dim, :] = (q + bias_col(bu_ref, h)).astype(BF16).astype(F32)
        rel_all = dot_nn(relp[...], rel[...])
        per_p = heads * slots
        sel = jnp.zeros((per_p, CHUNK), F32)
        for p in range(slots):
            sel = jnp.where(pos == p, rel_all[p * per_p:(p + 1) * per_p, :], sel)
        rels[...] = sel

        @pl.loop(0, heads)
        def _(h):
            r = aligned(h * e_dim, e_dim)
            qu = otr[r, :]
            k_new = qkv[aligned(he + h * e_dim, e_dim), cols].astype(F32)
            v_new = qkv[aligned(2 * he + h * e_dim, e_dim), cols].astype(F32)
            rel_h = rels[aligned(h * slots, slots), :]
            self_s = jnp.sum(qu * k_new, axis=0, keepdims=True)
            scores = []
            for j in range(slots):
                s = jnp.sum(qu * kc[h, j, :, cols].astype(F32), axis=0, keepdims=True)
                s = (jnp.where(pos == j, self_s, s) + rel_h[j:j + 1, :]) * scale
                scores.append(jnp.where(pos >= j, s, -1e30))
            top = functools.reduce(jnp.maximum, scores)
            exps = [jnp.exp(s - top) for s in scores]
            total = functools.reduce(jnp.add, exps)
            self_a = jnp.zeros_like(total)
            out = jnp.zeros((e_dim, CHUNK), F32)
            for j in range(slots):
                a = (exps[j] / total).astype(BF16).astype(F32)
                self_a = jnp.where(pos == j, a, self_a)
                out = out + jnp.where(pos > j, a, 0.0) * vc[h, j, :, cols].astype(F32)
            otr[r, :] = out + self_a * v_new

        obuf[cols, aligned(y * he, he)] = otr[...].T.astype(BF16)

    def project(pair):
        r = aligned(pair * PAIR, PAIR)
        hid[r, :] = tok[r, :].astype(F32) + dot_nn(obuf[r, :], wout[...])
        gain = gain_row(1)

        @pl.loop(0, PAIR // norm_rows)
        def _(i):
            q = aligned(pair * PAIR + i * norm_rows, norm_rows)
            m = norm(hid[q, :], gain)
            for k in range(n_x):
                normed[q, aligned(lax.rem(k - x + n_x, n_x) * wide, wide)] = m[:, k * wide:(k + 1) * wide]

    def gelu(v):
        half = 0.5 * v
        return half + half * jnp.tanh(v * (GELU_A + GELU_B * (v * v)))

    def up_rows(r, off, b):
        cols = aligned(b * blk, blk)
        w = wup[at_y(off), :, :, :, cols].reshape(d, blk)
        z[b, r, pl.ds(slot(off) * blk, blk)] = gelu(dot_nn(normed[r, :], w)).astype(BF16)

    def up_own(pair):
        @pl.loop(0, BLOCKS // 2)
        def _(i):
            for k in range(2):
                up_rows(aligned(pair * PAIR, PAIR), 0, 2 * i + k)

    def up_near(b, between=None):
        @pl.loop(0, n_tok // PAIR)
        def _(i):
            for off in (-1, 1):
                up_rows(aligned(i * PAIR, PAIR), off, b)
            if between is not None:
                pl.when(i == 0)(between)

    def down_rows(r, b, first, count):
        w = wdn[first:first + count, aligned(b * blk, blk), :].reshape(count * blk, d)
        hid[r, :] += dot_nn(z[b, r, first * blk:(first + count) * blk], w)

    def down_near(b):
        @pl.loop(0, n_tok // PAIR)
        def _(i):
            down_rows(aligned(i * PAIR, PAIR), b, 0, n_tp - 1)

    def far_down(b, first, between=None):
        @pl.loop(0, n_tok // PAIR)
        def _(i):
            r = aligned(i * PAIR, PAIR)
            up_rows(r, 2, b)
            down_rows(r, b, first, n_tp - first)
            if between is not None:
                pl.when(i == 0)(between)

    n_out = 4

    def last_block(b):
        up_rows(slice(None), 2, b)
        for i in range(n_out):
            cols = pl.ds(i * (d // n_out), d // n_out)
            w = wdn[:, b * blk:(b + 1) * blk, cols].reshape(n_tp * blk, d // n_out)
            y_out[:, cols] = (hid[:, cols] + dot_nn(z[b], w)).astype(BF16)

    @pl.loop(0, n_chunk)
    def _(ch):
        attend(ch)

        @pl.when(ch < 2)
        def _():
            y_own(("a", ch), o_view(ch))

        @pl.when(ch == 2)
        def _():
            x_relay("o", out_view)

    y_relay(("a", 0), o_view(0))
    y_own(("a", 2), o_view(2))
    x_relay("u", up_view)
    y_fin("dya", dny_view(0))
    y_fin("dyb", dny_view(1))
    x_own(("d", 0), dn_view(0))
    x_own(("d", 1), dn_view(1))
    y_relay(("a", 1), o_view(1))
    y_own(("a", 3), o_view(3))
    kn_out[...] = qkv[he:2 * he, :]
    vn_out[...] = qkv[2 * he:3 * he, :]
    x_fin("o", out_view)
    y_relay(("a", 2), o_view(2))
    y_relay("u0", u0_view, True)
    x_sib("o", out_view)

    @pl.loop(0, n_tok // PAIR)
    def _(p):
        for i in range(2):
            y_fin(("a", 2 * p + i), o_view(2 * p + i))
        project(p)

        @pl.when(p == 0)
        def _():
            x_fin("u", up_view)
            y_relay(("a", 3), o_view(3))
            y_own(("v", 0), ub_view(0))
            y_own(("v", 1), ub_view(1))
            x_sib("u", up_view)

        up_own(p)

        @pl.when(p == 0)
        def _():
            x_relay(("d", 0), dn_view(0))
            x_own(("d", 2), dn_view(2))

    y_sib_near("u0", u0_view)
    y_relay(("v", 0), ub_view(0), True)
    y_own(("v", 2), ub_view(2))
    x_relay(("d", 1), dn_view(1))
    x_own(("d", 3), dn_view(3))
    y_fin("u0", u0_view, True)
    x_fin(("d", 0), dn_view(0))
    y_sib_near(("v", 0), ub_view(0))
    up_near(0)
    y_relay(("v", 1), ub_view(1), True)
    y_own(("v", 3), ub_view(3))
    y_sib_far("u0", u0_view)
    x_sib(("d", 0), dn_view(0))
    down_near(0)

    @pl.loop(1, BLOCKS)
    def _(b):
        y_sib_near(("v", b), ub_view(b))
        up_near(b, lambda: y_fin(("v", b - 1), ub_view(b - 1), True))
        y_sib_far(("v", b - 1), ub_view(b - 1))

        @pl.when(b < BLOCKS - 1)
        def _():
            x_relay(("d", b + 1), dn_view(b + 1))

        def between():
            @pl.when(b < BLOCKS - 1)
            def _():
                y_relay(("v", b + 1), ub_view(b + 1), True)

            @pl.when(b == BLOCKS - 1)
            def _():
                y_fin(("v", b), ub_view(b), True)
                x_fin(("d", b), dn_view(b))

        @pl.when(b == 1)
        def _():
            far_down(0, n_tp - 1, between)

        @pl.when(b > 1)
        def _():
            x_sib(("d", b - 1), dn_view(b - 1))
            far_down(b - 1, 0, between)

        @pl.when(b < BLOCKS - 1)
        def _():
            x_fin(("d", b), dn_view(b))

    sent("g", "f", gbuf.at[pl.ds(0, 2 * n_x - 1)])
    for t, view in (("qa", qa_view), ("qb", qb_view), ("o", out_view), ("u", up_view)):
        x_sent(t, view)
    for t, view, share in (("oy", outy_view, False), ("dya", dny_view(0), False), ("dyb", dny_view(1), False), ("u0", u0_view, True)):
        y_sent(t, view, share)
    for b in range(BLOCKS):
        y_sent(("a", b), o_view(b))
        y_sent(("v", b), ub_view(b), True)
        x_sent(("d", b), dn_view(b))
    x_sib(("d", BLOCKS - 1), dn_view(BLOCKS - 1))
    y_sib_far(("v", BLOCKS - 1), ub_view(BLOCKS - 1))
    last_block(BLOCKS - 1)
    assert FAMILY_TENSORS + len(tensors) == TENSORS, len(tensors)
    assert FAMILY_ARRIVALS + len(arrivals) == ARRIVALS, len(arrivals)
    assert n_local[0] == MAX_LOCALS, n_local


def write_kernel(parts, *refs):
    n = (len(refs) - 1) // 2
    sems = refs[-1]
    puts = []
    for src, dst in zip(refs[:n], refs[n:2 * n]):
        rows = src.shape[0] // parts
        for i in range(parts):
            r = pl.ds(i * rows, rows)
            puts.append(pltpu.make_async_copy(src.at[r], dst.at[r], sems.at[len(puts)]))
    for put in puts:
        put.start()
    for put in puts:
        put.wait()


def solution(mesh):
    tok_axes = ("dp", "wg")
    in_specs = (P(tok_axes, None), P("wg"), P("wg"), P("wg", None, "tp", None), P("wg", "tp", None), P("tp", None, "wg"), P("wg", "tp"), P("tp", "wg"), P("tp", None), P("tp", None), P(None, None), P(tok_axes, "tp", None, None), P(tok_axes, "tp", None, None), P(tok_axes))
    out_specs = (P(tok_axes, None), P(tok_axes, "tp", None), P(tok_axes, "tp", None))
    n_wg, n_tp = mesh.shape["wg"], mesh.shape["tp"]

    def device_step(tokens, gain_attn, gain_mlp, w_qkv, w_rel, w_out, w_up, w_down, bias_u, bias_v, rel_table, k_cache, v_cache, positions):
        n_tok, d = tokens.shape
        _, heads, slots, e_dim = k_cache.shape
        he = heads * e_dim
        piece, f_loc = w_up.shape
        w_q = jnp.transpose(w_qkv, (1, 2, 3, 0)).reshape(3 * he, piece)
        w_r = jnp.transpose(w_rel, (1, 2, 0)).reshape(he, piece)
        w_o = w_out.reshape(he, piece)
        k_t = jnp.transpose(k_cache, (1, 2, 3, 0))
        v_t = jnp.transpose(v_cache, (1, 2, 3, 0))
        hbm = pl.BlockSpec(memory_space=pl.ANY)
        vmem = pl.BlockSpec(memory_space=pltpu.VMEM)
        y, k_new, v_new = pl.pallas_call(
            functools.partial(layer_kernel, n_wg, n_tp, (heads, slots, e_dim)),
            out_shape=(pltpu.VMEM((n_tok, d), BF16), pltpu.VMEM((he, n_tok), BF16), pltpu.VMEM((he, n_tok), BF16)),
            in_specs=[hbm] * 14,
            out_specs=(vmem, vmem, vmem),
            scratch_shapes=[
                pltpu.VMEM(bias_u.shape, F32),
                pltpu.VMEM(bias_v.shape, F32),
                pltpu.VMEM(rel_table.shape, BF16),
                pltpu.VMEM((1, n_tok), jnp.int32),
                pltpu.VMEM((n_tok, d), BF16),
                pltpu.VMEM(k_t.shape, BF16),
                pltpu.VMEM(v_t.shape, BF16),
                pltpu.VMEM((n_wg, 2, piece), F32),
                pltpu.VMEM((4 * he, d), BF16),
                pltpu.VMEM((n_tp * he, d), BF16),
                pltpu.VMEM((n_tp, n_wg // CORES, CORES, piece, f_loc), BF16),
                pltpu.VMEM((n_tp, f_loc, d), BF16),
                pltpu.VMEM((n_tok, d), BF16),
                pltpu.VMEM((3 * he, n_tok), BF16),
                pltpu.VMEM((he, CHUNK), BF16),
                pltpu.VMEM((slots * heads * slots, he), BF16),
                pltpu.VMEM((heads * slots, CHUNK), F32),
                pltpu.VMEM((n_tok, n_tp * he), BF16),
                pltpu.VMEM((he, CHUNK), F32),
                pltpu.VMEM((n_tok, d), F32),
                pltpu.VMEM((BLOCKS, n_tok, n_tp * (f_loc // BLOCKS)), BF16),
                pltpu.SemaphoreType.DMA((TENSORS,)),
                pltpu.SemaphoreType.DMA((ARRIVALS,)),
                pltpu.SemaphoreType.DMA((MAX_LOCALS,)),
            ],
            compiler_params=pltpu.CompilerParams(collective_id=0, has_side_effects=True, vmem_limit_bytes=KERNEL_VMEM),
            name="decoder_layer",
        )(tokens, gain_attn.reshape(1, piece), gain_mlp.reshape(1, piece), w_q, w_r, w_o, w_up, w_down, bias_u, bias_v, rel_table, k_t, v_t, positions.reshape(1, n_tok))
        results = (y, k_new, v_new)
        y, k_new, v_new = pl.pallas_call(
            functools.partial(write_kernel, PARTS),
            out_shape=tuple(jax.ShapeDtypeStruct(r.shape, r.dtype) for r in results),
            in_specs=[vmem] * len(results),
            out_specs=(hbm,) * len(results),
            scratch_shapes=[pltpu.SemaphoreType.DMA((PARTS * len(results),))],
            compiler_params=pltpu.CompilerParams(vmem_limit_bytes=4 << 20),
            name="write_results",
        )(*results)
        k_new = jnp.transpose(k_new.reshape(heads, e_dim, n_tok), (2, 0, 1))
        v_new = jnp.transpose(v_new.reshape(heads, e_dim, n_tok), (2, 0, 1))
        return y, k_new, v_new

    return jax.shard_map(device_step, mesh=mesh, in_specs=in_specs, out_specs=out_specs, check_vma=False)
```
